256 devices in a mesh: harm: 64 (over y, z, core), node: 4 (over x).
Axes of the slice: x: 4, y: 4, z: 8, core: 2. Of those that a mesh axis runs over, the one named last changes fastest.
Arguments:
- state: float32 [2, 128, 512, 128], P(None, 'harm', 'node'), may hold values from -0.6 to 0.6
- source: float32 [2, 128, 512, 128], P(None, 'harm', 'node'), may hold values from -6 to 6
- capacity: float32 [512, 128], P('node'), may hold values from 0.05 to 0.5
- row_shift: int32 [512], P('node'), may hold values from 0 to 3
- device_type: int32 [512, 128], P('node'), may hold values from 0 to 3
- device_table: float32 [3, 4], replicated, may hold values from 0.5 to 2
- precond: float32 [2, 128, 128, 128], P(None, 'harm'), may hold values from -1 to 1, as said below
Outputs:
- update: float32 [2, 128, 512, 128], P(None, 'harm', 'node')
- resid: float32 [2, 128, 512, 128], P(None, 'harm', 'node')
The draws below stay inside these ranges and needn't reach their ends.
Inputs may be any that keep to these rules, and one draw needn't show every extreme that they name: precond[0, k] is 1/6 on the diagonal plus a full-rank fluctuation; precond[1, k] is a full-rank fluctuation.
All inputs are finite; a program needn't handle non-finite values.
Results may differ from the reference program's by a relative error of at most 0.00011.
Values sent between devices are 32-bit elements; how exact they have to be, the bound alone decides.
A program may use at most 64 MiB of HBM per device.

```python
import math
import jax
import jax.numpy as jnp
from jax import lax

H = 128
S = 256
GY = 128
ITERS = 3
TYPES = 4
SHIFTS = 4
GX = 512


def draw_precond(key, part):
    first_key, second_key = jax.random.split(jax.random.fold_in(key, 17))
    noise_real = jnp.clip(jax.random.normal(first_key, (H, GY, GY), jnp.float32), -4.0, 4.0)
    noise_imag = jnp.clip(jax.random.normal(second_key, (H, GY, GY), jnp.float32), -4.0, 4.0)
    identity = jnp.eye(GY, dtype=jnp.float32)[None]
    real_part = (identity + 0.5 * noise_real / jnp.sqrt(GY * 1.0)) / 6.0
    imag_part = 0.5 * noise_imag / jnp.sqrt(GY * 1.0) / 6.0
    return jnp.stack([real_part, imag_part])


def set_ends(values, key, low, top_value):
    longest = values.shape.index(max(values.shape))
    spots = []
    for shift in (0, 1):
        where = [jax.random.randint(jax.random.fold_in(key, axis), (), 0, length) for axis, length in enumerate(values.shape)]
        where[longest] = (where[longest] + shift) % values.shape[longest]
        spots.append(tuple(where))
    return values.at[spots[0]].set(low).at[spots[1]].set(top_value)


def block_levels(stream_key, extent, cuts, low, largest):
    loudness = 1.0
    for axis_at, blocks in cuts:
        draws = jax.random.uniform(jax.random.fold_in(jax.random.fold_in(stream_key, 6), axis_at), (blocks,), jnp.float32, low / len(cuts), largest / len(cuts))
        loudness = loudness * jnp.repeat(jnp.exp(draws), extent[axis_at] // blocks).reshape((-1,) + (1,) * (len(extent) - 1 - axis_at))
    return loudness


def normal_values(key, shape, deviation, most, pieces=(), kind=jnp.bfloat16):
    values = deviation * jax.random.normal(key, shape, jnp.float32)
    if pieces:
        values = values * block_levels(key, shape, pieces, -0.22, 0.18)
    return jnp.clip(values, -most, most).astype(kind)


def setup_inputs(seed: int = 0) -> dict:
    keys = jax.random.split(jax.random.key(seed), 8)
    return {
        "state": normal_values(keys[0], (2, H, GX, GY), 0.1, 0.6, ((1, 64), (2, 4)), jnp.float32),
        "source": normal_values(keys[1], (2, H, GX, GY), 1.0, 6.0, ((1, 64), (2, 4)), jnp.float32),
        "capacity": jnp.clip(jnp.exp(math.log(0.5) - 2.3025851 * jax.random.uniform(keys[2], (GX, GY), jnp.float32) ** block_levels(keys[2], (GX, GY), ((0, 4),), -0.2, 0.2)), 0.05, 0.5),
        "row_shift": set_ends(jax.random.randint(keys[3], (GX,), 0, SHIFTS), jax.random.fold_in(keys[3], 1), 0, SHIFTS - 1).astype(jnp.int32),
        "device_type": set_ends(jax.random.randint(keys[4], (GX, GY), 0, TYPES), jax.random.fold_in(keys[4], 1), 0, TYPES - 1).astype(jnp.int32),
        "device_table": jnp.clip(jax.random.uniform(keys[5], (3, TYPES), jnp.float32, 0.5, 2.0), 0.5, 2.0),
        "precond": draw_precond(jax.random.fold_in(keys[7], 71), 0),
    }


omega_step = 0.05
top = lax.Precision.HIGHEST

def small_solve(gram, right):
    lower = jnp.linalg.cholesky(gram)
    order = gram.shape[0]
    forward = []
    for column in range(order):
        value = right[column]
        for member in range(column):
            value = value - lower[column, member] * forward[member]
        forward.append(value / lower[column, column])
    result = [None] * order
    for column in reversed(range(order)):
        value = forward[column]
        for member in range(column + 1, order):
            value = value - lower[member, column] * result[member]
        result[column] = value / lower[column, column]
    return result

def weights_of():
    waves = jnp.arange(H)
    return jnp.where(waves == 0, 1.0, 2.0).astype(jnp.float32)

def to_time(spectrum):
    scaled = (spectrum[0] + 1j * spectrum[1]) * (S / weights_of())[:, None, None]
    padded = jnp.concatenate([scaled, jnp.zeros((1,) + scaled.shape[1:], scaled.dtype)], axis=0)
    return jnp.fft.irfft(padded, n=S, axis=0)

def to_spec(signal):
    trans = jnp.fft.rfft(signal, axis=0)[:H]
    factor = (weights_of() / S)[:, None, None]
    return jnp.stack([jnp.real(trans) * factor, jnp.imag(trans) * factor])

def stencil(field, capacity, row_shift):
    left_side = jnp.roll(field, 1, axis=3)
    right_side = jnp.roll(field, -1, axis=3)
    zero_row = jnp.zeros(field.shape[:2] + (1, field.shape[3]), jnp.float32)
    above = jnp.concatenate([zero_row, field[:, :, :-1]], axis=2)
    below = jnp.concatenate([field[:, :, 1:], zero_row], axis=2)
    skewed = jnp.zeros_like(field)
    for amount in range(SHIFTS):
        picked = (row_shift == amount).astype(jnp.float32)[None, None, :, None]
        skewed = skewed + picked * jnp.roll(above, -amount, axis=3)
    result = 4.0 * field - left_side - right_side - skewed - below
    waves = jnp.arange(H).astype(jnp.float32)
    reactive = omega_step * waves[:, None, None] * capacity[None]
    return result + jnp.stack([-reactive * field[1], reactive * field[0]])

def precondition(field, blocks):
    real_part = jnp.einsum('krd,kcd->krc', field[0], blocks[0], precision=top) - jnp.einsum('krd,kcd->krc', field[1], blocks[1], precision=top)
    imag_part = jnp.einsum('krd,kcd->krc', field[0], blocks[1], precision=top) + jnp.einsum('krd,kcd->krc', field[1], blocks[0], precision=top)
    return jnp.stack([real_part, imag_part])

def reference(state, source, capacity, row_shift, device_type, device_table, precond):
    params = jnp.zeros((3,) + device_type.shape, jnp.float32)
    for member in range(TYPES):
        params = params + (device_type == member).astype(jnp.float32)[None] * device_table[:, member][:, None, None]
    linear, amplitude, slope = (params[0], params[1], params[2])
    voltage = to_time(state)
    bent = jnp.tanh(slope * voltage)
    flow = linear * voltage + amplitude * bent
    slopes = linear + amplitude * slope * (1.0 - bent * bent)
    resid = stencil(state, capacity, row_shift) + to_spec(flow) - source
    start = -resid
    beta = jnp.sqrt(jnp.sum(start * start))
    basis = [start / beta]
    directions = []
    columns_h = []
    for iteration in range(ITERS):
        direction = precondition(basis[iteration], precond)
        directions.append(direction)
        image = stencil(direction, capacity, row_shift) + to_spec(slopes * to_time(direction))
        heights = []
        for earlier in range(iteration + 1):
            height = jnp.sum(basis[earlier] * image)
            image = image - height * basis[earlier]
            heights.append(height)
        length = jnp.sqrt(jnp.sum(image * image))
        columns_h.append(jnp.stack(heights + [length] + [jnp.zeros((), jnp.float32)] * (ITERS - 1 - iteration)))
        if iteration + 1 < ITERS:
            basis.append(image / length)
    hess = jnp.stack(columns_h, axis=1)
    gram = jnp.dot(hess.T, hess, precision=top)
    coeffs = small_solve(gram, beta * hess[0])
    update = jnp.zeros_like(state)
    for iteration in range(ITERS):
        update = update + coeffs[iteration] * directions[iteration]
    return (update, resid)
```

```python
import functools

import jax
import jax.numpy as jnp
import numpy as np
from jax import lax
from jax.experimental import pallas as pl
from jax.experimental.pallas import tpu as pltpu
from jax.sharding import PartitionSpec as P

ITERS = 3
TYPES = 4
SHIFTS = 4
OMEGA = 0.05
MESH = pl.DeviceIdType.MESH
F32 = jnp.float32
BF16 = jnp.bfloat16


def split(x):
    high = x.astype(BF16)
    low = (x - high.astype(F32)).astype(BF16)
    return high, low


def tables(harmonics):
    samples = 2 * harmonics
    row = np.arange(2 * harmonics)
    wave = (row // 4) * 2 + row % 2
    part = (row // 2) % 2
    moment = np.arange(samples)
    phase = (moment[:, None] * wave[None, :] % samples) * (2.0 * np.pi / samples)
    inverse = np.where(part[None, :] == 0, np.cos(phase), -np.sin(phase))
    weight = np.where(wave == 0, 1.0, 2.0) / samples
    forward = inverse.T * weight[:, None]

    def stacked(matrix):
        matrix = matrix.astype(np.float32)
        high = matrix.astype(jnp.bfloat16)
        low = (matrix - high.astype(np.float32)).astype(jnp.bfloat16)
        return np.concatenate([high, low, high], axis=1)

    return stacked(inverse), stacked(forward)


def kernel(
    state_hbm, source_hbm, cap_hbm, shift_hbm, kinds_hbm, table, precond_hbm, inv_hbm, fwd_hbm,
    update_hbm, resid_hbm,
    state, source, cap, shift, kinds, precond, inv, fwd,
    weights, slopes, basis, images, directions, out_update, out_resid,
    t_send, t_recv, l_send, l_recv, halo_send, halo_recv, ar_send, ar_recv, ax_send, ax_recv,
    in_sem, out_sem, t_ssem, t_rsem, l_ssem, l_rsem, h_ssem, h_rsem, a_ssem, a_rsem, x_ssem, x_rsem,
):
    harm = lax.axis_index("harm")
    node = lax.axis_index("node")
    y, z, core = harm // 16, lax.rem(harm // 2, 8), lax.rem(harm, 2)
    inputs = [
        (state_hbm, state), (inv_hbm, inv), (kinds_hbm, kinds), (fwd_hbm, fwd),
        (precond_hbm, precond), (shift_hbm, shift), (cap_hbm, cap), (source_hbm, source),
    ]
    loads = [pltpu.make_async_copy(a, b, in_sem.at[i]) for i, (a, b) in enumerate(inputs)]
    for load in loads:
        load.start()

    def peer(j):
        i, jy, jc = j // 8, lax.rem(j // 2, 4), lax.rem(j, 2)
        dz = jnp.where(lax.rem(i, 2) == 0, 4 + i // 2, 4 - (i + 1) // 2)
        dy = jnp.where(lax.rem(jy, 2) == 0, 2 + jy // 2, 2 - (jy + 1) // 2)
        dc = 1 - jc
        return lax.rem(y + dy, 4) * 16 + lax.rem(z + dz, 8) * 2 + lax.rem(core + dc, 2)

    barrier = pltpu.get_barrier_semaphore()

    @pl.loop(0, 63)
    def _(j):
        pl.semaphore_signal(barrier, inc=1, device_id=(peer(j), node), device_id_type=MESH)

    for d in (1, 2, 3):
        pl.semaphore_signal(
            barrier, inc=1, device_id=(harm, lax.rem(node + d, 4)), device_id_type=MESH
        )

    def tile(index):
        return pl.ds(pl.multiple_of(index * 8, 8), 8)

    def exchange(send, recv, ssem, rsem, stage):
        @pl.loop(0, 63)
        def _(j):
            other = peer(j)
            pltpu.make_async_remote_copy(
                src_ref=send.at[stage, tile(other)],
                dst_ref=recv.at[stage, tile(harm)],
                send_sem=ssem.at[stage],
                recv_sem=rsem.at[stage],
                device_id=(other, node),
                device_id_type=MESH,
            ).start()

        recv[stage, tile(harm), :] = send[stage, tile(harm), :]

    def arrived(send, recv, ssem, rsem, stage):
        return pltpu.make_async_remote_copy(
            src_ref=send.at[stage, pl.ds(0, 504)],
            dst_ref=recv.at[stage, pl.ds(0, 504)],
            send_sem=ssem.at[stage],
            recv_sem=rsem.at[stage],
            device_id=(lax.rem(harm + 1, 64), node),
            device_id_type=MESH,
        )

    t_all = (t_send, t_recv, t_ssem, t_rsem)
    l_all = (l_send, l_recv, l_ssem, l_rsem)

    def halo_copy(stage, side):
        step = 1 if side == 0 else 3
        return pltpu.make_async_remote_copy(
            src_ref=halo_send.at[stage, side],
            dst_ref=halo_recv.at[stage, side],
            send_sem=h_ssem.at[stage, side],
            recv_sem=h_rsem.at[stage, side],
            device_id=(harm, lax.rem(node + step, 4)),
            device_id_type=MESH,
        )

    pairs = [(p, kk) for p in range(2) for kk in range(2)]

    def to_time(field, stage):
        for p, kk in pairs:
            for i in range(2):
                q = (p * 2 + kk) * 2 + i
                t_send[stage, pl.ds(q, 64, stride=8), :] = field[p, kk, i * 64 : (i + 1) * 64, :]
        last = [field[p, kk, 127:128, :] for p, kk in pairs]
        first = [field[p, kk, 0:1, :] for p, kk in pairs]
        halo_send[stage, 0] = jnp.concatenate(last + last, axis=0)
        halo_send[stage, 1] = jnp.concatenate(first + first, axis=0)

    def depart(stage):
        exchange(*t_all, stage)
        for side in range(2):
            halo_copy(stage, side).start()

    def rhs(x):
        high, low = split(x)
        return jnp.concatenate([high, high, low], axis=0)

    def time_of(stage):
        u = jnp.concatenate(
            [t_recv[stage, pl.ds(i, 256, stride=2), :] for i in range(2)], axis=1
        )
        return jnp.dot(inv[...], rhs(u), preferred_element_type=F32)

    def to_spec(signal, stage):
        spec = jnp.dot(fwd[...], rhs(signal), preferred_element_type=F32)
        for i in range(2):
            l_send[stage, pl.ds(i, 256, stride=2), :] = spec[:, i * 128 : (i + 1) * 128]
        exchange(*l_all, stage)

    def spec_part(stage, p, kk):
        q = (p * 2 + kk) * 2
        return jnp.concatenate(
            [l_recv[stage, pl.ds(q + i, 64, stride=8), :] for i in range(2)], axis=0
        )

    loads[0].wait()
    to_time(state, 0)
    pl.semaphore_wait(barrier, 66)
    depart(0)

    for load in loads[1:]:
        load.wait()
    for kk in range(2):
        real, imag = precond[0, kk].T, precond[1, kk].T
        whole = jnp.concatenate(
            [jnp.concatenate([real, imag], axis=1), jnp.concatenate([-imag, real], axis=1)], axis=0
        )
        high, low = split(whole)
        weights[kk, 0:256, :] = high
        weights[kk, 256:512, :] = high
        weights[kk, 512:768, :] = low
    kind = jnp.concatenate([kinds[pl.ds(harm, 1), :], kinds[pl.ds(harm + 64, 1), :]], axis=1)
    linear, amplitude, slope = [
        sum(jnp.where(kind == member, table[what, member], 0.0) for member in range(TYPES))
        for what in range(3)
    ]
    shifts = jnp.broadcast_to(shift[...].astype(F32), (128, 128)).T
    row = lax.broadcasted_iota(jnp.int32, (128, 128), 0)
    waves = [(2 * harm + kk).astype(F32) * OMEGA for kk in range(2)]
    not_first = jnp.where(node == 0, 0.0, 1.0)
    not_last = jnp.where(node == 3, 0.0, 1.0)

    def stencil(field, stage, p, kk):
        f = field[p, kk]
        index = p * 2 + kk
        halo_a = halo_recv[stage, 0, index : index + 1, :] * not_first
        halo_b = halo_recv[stage, 1, index : index + 1, :] * not_last
        above = jnp.where(row == 0, halo_a, pltpu.roll(f, 1, axis=0))
        below = jnp.where(row == 127, halo_b, pltpu.roll(f, 127, axis=0))
        skewed = above
        for amount in range(1, SHIFTS):
            skewed = jnp.where(
                shifts == float(amount), pltpu.roll(above, 128 - amount, axis=1), skewed
            )
        sides = pltpu.roll(f, 1, axis=1) + pltpu.roll(f, 127, axis=1)
        result = 4.0 * f - sides - skewed - below
        turned = waves[kk] * cap[...] * field[1 - p, kk]
        return result - turned if p == 0 else result + turned

    def halo_wait(stage):
        for side in range(2):
            halo_copy(stage, side).wait_recv()

    def precondition(field, target):
        for kk in range(2):
            high, low = split(jnp.concatenate([field[0, kk], field[1, kk]], axis=1))
            both = jnp.dot(
                jnp.concatenate([high, low, high], axis=1),
                weights[kk],
                preferred_element_type=F32,
            )
            target[0, kk] = both[:, 0:128]
            target[1, kk] = both[:, 128:256]

    lane = lax.broadcasted_iota(jnp.int32, (1, 128), 1)

    def inner(a, b):
        total = sum(a[p, kk] * b[p, kk] for p, kk in pairs)
        return jnp.sum(jnp.sum(total, axis=0, keepdims=True), axis=1, keepdims=True)

    def reduce_start(stage, values):
        packed = sum(jnp.where(lane == q, value, 0.0) for q, value in enumerate(values))
        ar_send[stage] = packed

        @pl.loop(0, 63)
        def _(j):
            pltpu.make_async_remote_copy(
                src_ref=ar_send.at[stage],
                dst_ref=ar_recv.at[stage, harm],
                send_sem=a_ssem.at[stage],
                recv_sem=a_rsem.at[stage],
                device_id=(peer(j), node),
                device_id_type=MESH,
            ).start()

        ar_recv[stage, harm] = packed

    def reduce_all(stage):
        return pltpu.make_async_remote_copy(
            src_ref=ar_recv.at[stage, pl.ds(0, 63)],
            dst_ref=ar_recv.at[stage, pl.ds(0, 63)],
            send_sem=a_ssem.at[stage],
            recv_sem=a_rsem.at[stage],
            device_id=(lax.rem(harm + 1, 64), node),
            device_id_type=MESH,
        )

    def ax_copy(stage, d):
        return pltpu.make_async_remote_copy(
            src_ref=ax_send.at[stage],
            dst_ref=ax_recv.at[stage, node],
            send_sem=x_ssem.at[stage, d],
            recv_sem=x_rsem.at[stage, d],
            device_id=(harm, lax.rem(node + d + 1, 4)),
            device_id_type=MESH,
        )

    def reduce_middle(stage):
        reduce_all(stage).wait_recv()
        total = jnp.sum(ar_recv[stage], axis=0)
        ax_send[stage] = total
        for d in range(3):
            ax_copy(stage, d).start()
        ax_recv[stage, node] = total

    def reduce_finish(stage):
        for d in range(3):
            ax_copy(stage, d).wait_recv()
        total = jnp.sum(ax_recv[stage], axis=0)
        return lambda q: total[:, q : q + 1]

    arrived(*t_all, 0).wait_recv()
    voltage = time_of(0)
    bent = jnp.tanh(slope * voltage)
    slopes[...] = linear + amplitude * slope * (1.0 - bent * bent)
    to_spec(linear * voltage + amplitude * bent, 0)
    halo_wait(0)
    p0, p1 = basis.at[0], basis.at[1]
    for p, kk in pairs:
        basis[0, p, kk] = source[p, kk] - stencil(state, 0, p, kk)
    arrived(*l_all, 0).wait_recv()
    for p, kk in pairs:
        start = basis[0, p, kk] - spec_part(0, p, kk)
        basis[0, p, kk] = start
        out_resid[p, kk] = -start
    resid_out = pltpu.make_async_copy(out_resid, resid_hbm, out_sem.at[0])
    resid_out.start()

    def send_direction(source_ref, stage):
        precondition(source_ref, directions.at[stage - 1])
        to_time(directions.at[stage - 1], stage)
        depart(stage)

    def apply_time(stage):
        arrived(*t_all, stage).wait_recv()
        to_spec(slopes[...] * time_of(stage), stage)

    def local_image(stage):
        halo_wait(stage)
        for p, kk in pairs:
            images[stage - 1, p, kk] = stencil(directions.at[stage - 1], stage, p, kk)

    send_direction(p0, 1)
    apply_time(1)
    local_image(1)
    arrived(*l_all, 1).wait_recv()
    for p, kk in pairs:
        images[0, p, kk] = images[0, p, kk] + spec_part(1, p, kk)
    z0, z1, z2 = [directions.at[j] for j in range(3)]
    i0, i1, i2 = [images.at[j] for j in range(3)]

    send_direction(i0, 2)
    reduce_start(0, [inner(p0, p0), inner(p0, i0), inner(i0, i0)])
    apply_time(2)
    local_image(2)
    reduce_middle(0)
    first = reduce_finish(0)
    h = first(1) / first(0)
    for p, kk in pairs:
        basis[1, p, kk] = i0[p, kk] - h * p0[p, kk]
        directions[1, p, kk] = z1[p, kk] - h * z0[p, kk]
        images[1, p, kk] = i1[p, kk] - h * i0[p, kk]
    arrived(*l_all, 2).wait_recv()
    for p, kk in pairs:
        images[1, p, kk] = images[1, p, kk] + spec_part(2, p, kk)

    send_direction(i1, 3)
    reduce_start(
        1, [inner(p0, i1), inner(p1, i1), inner(p1, p1), inner(i0, i1), inner(i1, i1)]
    )
    apply_time(3)
    local_image(3)
    reduce_middle(1)
    second = reduce_finish(1)
    h0, h1 = second(0) / first(0), second(1) / second(2)
    for p, kk in pairs:
        directions[2, p, kk] = z2[p, kk] - h0 * z0[p, kk] - h1 * z1[p, kk]
        images[2, p, kk] = i2[p, kk] - h0 * i0[p, kk] - h1 * i1[p, kk]
    arrived(*l_all, 3).wait_recv()
    for p, kk in pairs:
        images[2, p, kk] = images[2, p, kk] + spec_part(3, p, kk)
    reduce_start(2, [inner(p0, i2), inner(i0, i2), inner(i1, i2), inner(i2, i2)])
    reduce_middle(2)
    third = reduce_finish(2)

    g00, g01, g02 = first(2), second(3), third(1)
    g11, g12, g22 = second(4), third(2), third(3)
    b0, b1, b2 = first(1), second(0), third(0)
    l10, l20 = g01 / g00, g02 / g00
    d1 = g11 - l10 * g01
    e12 = g12 - l10 * g02
    c1 = b1 - l10 * b0
    l21 = e12 / d1
    d2 = g22 - l20 * g02 - l21 * e12
    c2 = b2 - l20 * b0 - l21 * c1
    y2 = c2 / d2
    y1 = (c1 - e12 * y2) / d1
    y0 = (b0 - g01 * y1 - g02 * y2) / g00
    for p, kk in pairs:
        out_update[p, kk] = y0 * z0[p, kk] + y1 * z1[p, kk] + y2 * z2[p, kk]
    update_out = pltpu.make_async_copy(out_update, update_hbm, out_sem.at[1])
    update_out.start()

    for stage in range(4):
        arrived(*t_all, stage).wait_send()
        arrived(*l_all, stage).wait_send()
        for side in range(2):
            halo_copy(stage, side).wait_send()
    for stage in range(3):
        reduce_all(stage).wait_send()
        for d in range(3):
            ax_copy(stage, d).wait_send()
    resid_out.wait()
    update_out.wait()


def body(state, source, capacity, row_shift, device_type, device_table, precond):
    inverse, forward = tables(state.shape[1] * lax.axis_size("harm"))
    block = (2, 2, 128, 128)
    vmem = pltpu.VMEM
    dma = pltpu.SemaphoreType.DMA
    hbm = pl.BlockSpec(memory_space=pl.ANY)
    update, resid = pl.pallas_call(
        kernel,
        out_shape=[jax.ShapeDtypeStruct(block, F32)] * 2,
        in_specs=[hbm] * 5 + [pl.BlockSpec(memory_space=pltpu.SMEM)] + [hbm] * 3,
        out_specs=[hbm, hbm],
        scratch_shapes=[
            vmem(block, F32), vmem(block, F32), vmem((128, 128), F32), vmem((1, 128), jnp.int32),
            vmem((128, 128), jnp.int32), vmem(block, F32), vmem((256, 768), BF16),
            vmem((256, 768), BF16),
            vmem((2, 768, 256), BF16), vmem((256, 256), F32), vmem((2,) + block, F32),
            vmem((3,) + block, F32), vmem((3,) + block, F32), vmem(block, F32), vmem(block, F32),
            vmem((4, 512, 128), F32), vmem((4, 512, 128), F32),
            vmem((4, 512, 128), F32), vmem((4, 512, 128), F32),
            vmem((4, 2, 8, 128), F32), vmem((4, 2, 8, 128), F32),
            vmem((3, 1, 128), F32), vmem((3, 64, 1, 128), F32),
            vmem((3, 1, 128), F32), vmem((3, 4, 1, 128), F32),
            dma((8,)), dma((2,)), dma((4,)), dma((4,)), dma((4,)), dma((4,)),
            dma((4, 2)), dma((4, 2)), dma((3,)), dma((3,)), dma((3, 3)), dma((3, 3)),
        ],
        compiler_params=pltpu.CompilerParams(
            collective_id=0, has_side_effects=True, vmem_limit_bytes=40 * 2**20
        ),
    )(
        state, source, capacity, row_shift.reshape(1, -1), device_type, device_table, precond,
        jnp.asarray(inverse), jnp.asarray(forward),
    )
    return update, resid


def solution(mesh):
    harm, node = mesh.axis_names
    return jax.shard_map(
        body,
        mesh=mesh,
        in_specs=(
            P(None, harm, node, None),
            P(None, harm, node, None),
            P(node, None),
            P(node),
            P(node, None),
            P(),
            P(None, harm, None, None),
        ),
        out_specs=(P(None, harm, node, None), P(None, harm, node, None)),
        check_vma=False,
    )
```

```python
import functools

import jax
import jax.numpy as jnp
import numpy as np
from jax import lax
from jax.experimental import pallas as pl
from jax.experimental.pallas import tpu as pltpu
from jax.sharding import PartitionSpec as P

ITERS = 3
TYPES = 4
SHIFTS = 4
OMEGA = 0.05
MESH = pl.DeviceIdType.MESH
F32 = jnp.float32
BF16 = jnp.bfloat16


def split(x):
    high = x.astype(BF16)
    low = (x - high.astype(F32)).astype(BF16)
    return high, low


def tables(harmonics):
    samples = 2 * harmonics
    row = np.arange(2 * harmonics)
    wave = (row // 4) * 2 + row % 2
    part = (row // 2) % 2
    moment = np.arange(samples)
    phase = (moment[:, None] * wave[None, :] % samples) * (2.0 * np.pi / samples)
    inverse = np.where(part[None, :] == 0, np.cos(phase), -np.sin(phase))
    weight = np.where(wave == 0, 1.0, 2.0) / samples
    forward = inverse.T * weight[:, None]

    def stacked(matrix):
        matrix = matrix.astype(np.float32)
        high = matrix.astype(jnp.bfloat16)
        low = (matrix - high.astype(np.float32)).astype(jnp.bfloat16)
        return np.concatenate([high, low], axis=0)

    return stacked(inverse), stacked(forward)


def kernel(
    state_hbm, source_hbm, cap_hbm, shift_hbm, kinds_hbm, table, precond_hbm, inv_hbm, fwd_hbm,
    out_update, out_resid,
    state, source, cap, shift, kinds, precond, inv, fwd,
    weights, slopes, basis, images, directions,
    t_send, t_recv, l_send, l_recv, halo_send, halo_recv, ar_send, ar_recv, ax_send, ax_recv,
    in_sem, t_ssem, t_rsem, l_ssem, l_rsem, h_ssem, h_rsem, a_ssem, a_rsem, x_ssem, x_rsem,
):
    harm = lax.axis_index("harm")
    node = lax.axis_index("node")
    y, z, core = harm // 16, lax.rem(harm // 2, 8), lax.rem(harm, 2)
    inputs = [
        (state_hbm, state), (inv_hbm, inv), (kinds_hbm, kinds), (fwd_hbm, fwd),
        (precond_hbm, precond), (shift_hbm, shift), (cap_hbm, cap), (source_hbm, source),
    ]
    loads = [pltpu.make_async_copy(a, b, in_sem.at[i]) for i, (a, b) in enumerate(inputs)]
    for load in loads:
        load.start()

    y_parts = [lax.rem(y + dy, 4) * 16 for dy in range(4)]
    c_parts = [lax.rem(core + dc, 2) for dc in range(2)]
    near = [(dy, dc) for dy in (2, 1, 3, 0) for dc in (1, 0)]

    def each_peer(act):
        @pl.loop(0, 7)
        def _(i):
            dz = jnp.where(lax.rem(i, 2) == 0, 4 + i // 2, 4 - (i + 1) // 2)
            z_part = lax.rem(z + dz, 8) * 2
            for dy, dc in near:
                act(y_parts[dy] + z_part + c_parts[dc])

        for dy, dc in near[:-1]:
            act(y_parts[dy] + z * 2 + c_parts[dc])

    barrier = pltpu.get_barrier_semaphore()

    def greet(other):
        pl.semaphore_signal(barrier, inc=1, device_id=(other, node), device_id_type=MESH)

    each_peer(greet)
    for d in (1, 2, 3):
        pl.semaphore_signal(
            barrier, inc=1, device_id=(harm, lax.rem(node + d, 4)), device_id_type=MESH
        )

    def unit(index):
        return pl.ds(pl.multiple_of(index * 4, 4), 4)

    def exchange(send, recv, ssem, rsem, stage, half):
        def push(other):
            pltpu.make_async_remote_copy(
                src_ref=send.at[stage, half, unit(other)],
                dst_ref=recv.at[stage, half, unit(harm)],
                send_sem=ssem.at[stage, half],
                recv_sem=rsem.at[stage, half],
                device_id=(other, node),
                device_id_type=MESH,
            ).start()

        each_peer(push)
        recv[stage, half, unit(harm), :] = send[stage, half, unit(harm), :]

    def arrived(send, recv, ssem, rsem, stage, half):
        return pltpu.make_async_remote_copy(
            src_ref=send.at[stage, half, pl.ds(0, 252)],
            dst_ref=recv.at[stage, half, pl.ds(0, 252)],
            send_sem=ssem.at[stage, half],
            recv_sem=rsem.at[stage, half],
            device_id=(lax.rem(harm + 1, 64), node),
            device_id_type=MESH,
        )

    t_all = (t_send, t_recv, t_ssem, t_rsem)
    l_all = (l_send, l_recv, l_ssem, l_rsem)

    def halo_copy(stage, side):
        step = 1 if side == 0 else 3
        return pltpu.make_async_remote_copy(
            src_ref=halo_send.at[stage, side],
            dst_ref=halo_recv.at[stage, side],
            send_sem=h_ssem.at[stage, side],
            recv_sem=h_rsem.at[stage, side],
            device_id=(harm, lax.rem(node + step, 4)),
            device_id_type=MESH,
        )

    pairs = [(p, kk) for p in range(2) for kk in range(2)]
    halves = [slice(0, 64), slice(64, 128)]

    def to_time(field, stage, half):
        for p, kk in pairs:
            t_send[stage, half, pl.ds(p * 2 + kk, 64, stride=4), :] = field[p, kk, halves[half], :]

    def send_halo(field, stage):
        last = [field[p, kk, 127:128, :] for p, kk in pairs]
        first = [field[p, kk, 0:1, :] for p, kk in pairs]
        halo_send[stage, 0] = jnp.concatenate(last + last, axis=0)
        halo_send[stage, 1] = jnp.concatenate(first + first, axis=0)
        for side in range(2):
            halo_copy(stage, side).start()

    def product(matrix, x):
        high, low = split(x)
        all_parts = jnp.dot(
            matrix[...], jnp.concatenate([high, low], axis=1), preferred_element_type=F32
        )
        return (all_parts[0:256, 0:128] + all_parts[0:256, 128:256]) + all_parts[256:512, 0:128]

    def time_of(stage, half):
        return product(inv, t_recv[stage, half])

    def to_spec(signal, stage, half):
        l_send[stage, half] = product(fwd, signal)
        exchange(*l_all, stage, half)

    def spec_part(stage, half, p, kk):
        return l_recv[stage, half, pl.ds(p * 2 + kk, 64, stride=4), :]

    loads[0].wait()
    to_time(state, 0, 0)
    pl.semaphore_wait(barrier, 66)
    exchange(*t_all, 0, 0)
    to_time(state, 0, 1)
    exchange(*t_all, 0, 1)
    send_halo(state, 0)

    for load in loads[1:]:
        load.wait()
    for kk in range(2):
        both = jnp.concatenate([precond[0, kk].T, precond[1, kk].T], axis=1)
        high, low = split(both)
        weights[kk, 0:128, :] = high
        weights[kk, 128:256, :] = low
    params = []
    for half in range(2):
        kind = kinds[pl.ds(harm + half * 64, 1), :]
        params.append(
            [
                sum(jnp.where(kind == member, table[what, member], 0.0) for member in range(TYPES))
                for what in range(3)
            ]
        )
    shifts = jnp.broadcast_to(shift[...].astype(F32), (128, 128)).T
    row = lax.broadcasted_iota(jnp.int32, (128, 128), 0)
    waves = [(2 * harm + kk).astype(F32) * OMEGA for kk in range(2)]
    not_first = jnp.where(node == 0, 0.0, 1.0)
    not_last = jnp.where(node == 3, 0.0, 1.0)

    def stencil(field, stage, p, kk):
        f = field[p, kk]
        index = p * 2 + kk
        halo_a = halo_recv[stage, 0, index : index + 1, :] * not_first
        halo_b = halo_recv[stage, 1, index : index + 1, :] * not_last
        above = jnp.where(row == 0, halo_a, pltpu.roll(f, 1, axis=0))
        below = jnp.where(row == 127, halo_b, pltpu.roll(f, 127, axis=0))
        skewed = above
        for amount in range(1, SHIFTS):
            skewed = jnp.where(
                shifts == float(amount), pltpu.roll(above, 128 - amount, axis=1), skewed
            )
        sides = pltpu.roll(f, 1, axis=1) + pltpu.roll(f, 127, axis=1)
        result = 4.0 * f - sides - skewed - below
        turned = waves[kk] * cap[...] * field[1 - p, kk]
        return result - turned if p == 0 else result + turned

    def halo_wait(stage):
        for side in range(2):
            halo_copy(stage, side).wait_recv()

    zero = jnp.zeros((128, 128), BF16)

    def precondition(field, target, half):
        part = halves[half]
        for kk in range(2):
            high, low = split(
                jnp.concatenate([field[0, kk, part, :], field[1, kk, part, :]], axis=0)
            )
            left = jnp.concatenate(
                [
                    jnp.concatenate([high, high], axis=1),
                    jnp.concatenate([low, zero], axis=1),
                ],
                axis=0,
            )
            out = jnp.dot(left, weights[kk], preferred_element_type=F32)
            out = out[0:128] + out[128:256]
            target[0, kk, part, :] = out[0:64, 0:128] - out[64:128, 128:256]
            target[1, kk, part, :] = out[0:64, 128:256] + out[64:128, 0:128]

    lane = lax.broadcasted_iota(jnp.int32, (1, 128), 1)

    def inner(a, b):
        total = sum(a[p, kk] * b[p, kk] for p, kk in pairs)
        return jnp.sum(jnp.sum(total, axis=0, keepdims=True), axis=1, keepdims=True)

    def reduce_start(stage, values):
        packed = sum(jnp.where(lane == q, value, 0.0) for q, value in enumerate(values))
        ar_send[stage] = packed

        def push(other):
            pltpu.make_async_remote_copy(
                src_ref=ar_send.at[stage],
                dst_ref=ar_recv.at[stage, harm],
                send_sem=a_ssem.at[stage],
                recv_sem=a_rsem.at[stage],
                device_id=(other, node),
                device_id_type=MESH,
            ).start()

        each_peer(push)
        ar_recv[stage, harm] = packed

    def reduce_all(stage):
        return pltpu.make_async_remote_copy(
            src_ref=ar_recv.at[stage, pl.ds(0, 63)],
            dst_ref=ar_recv.at[stage, pl.ds(0, 63)],
            send_sem=a_ssem.at[stage],
            recv_sem=a_rsem.at[stage],
            device_id=(lax.rem(harm + 1, 64), node),
            device_id_type=MESH,
        )

    def ax_copy(stage, d):
        return pltpu.make_async_remote_copy(
            src_ref=ax_send.at[stage],
            dst_ref=ax_recv.at[stage, node],
            send_sem=x_ssem.at[stage, d],
            recv_sem=x_rsem.at[stage, d],
            device_id=(harm, lax.rem(node + d + 1, 4)),
            device_id_type=MESH,
        )

    def reduce_middle(stage):
        reduce_all(stage).wait_recv()
        total = jnp.sum(ar_recv[stage], axis=0)
        ax_send[stage] = total
        for d in range(3):
            ax_copy(stage, d).start()
        ax_recv[stage, node] = total

    def reduce_finish(stage):
        for d in range(3):
            ax_copy(stage, d).wait_recv()
        total = jnp.sum(ax_recv[stage], axis=0)
        return lambda q: total[:, q : q + 1]

    def evaluate(half):
        linear, amplitude, slope = params[half]
        arrived(*t_all, 0, half).wait_recv()
        voltage = time_of(0, half)
        bent = jnp.tanh(slope * voltage)
        slopes[half] = linear + amplitude * slope * (1.0 - bent * bent)
        to_spec(linear * voltage + amplitude * bent, 0, half)

    p0 = basis.at[0]
    evaluate(0)
    halo_wait(0)
    for p, kk in pairs:
        basis[0, p, kk] = source[p, kk] - stencil(state, 0, p, kk)
    evaluate(1)
    z0, z1, z2 = [directions.at[j] for j in range(3)]
    i0, i1, i2 = [images.at[j] for j in range(3)]
    for half, part in enumerate(halves):
        arrived(*l_all, 0, half).wait_recv()
        for p, kk in pairs:
            basis[0, p, kk, part, :] = basis[0, p, kk, part, :] - spec_part(0, half, p, kk)
        precondition(p0, z0, half)
        to_time(z0, 1, half)
        exchange(*t_all, 1, half)
    send_halo(z0, 1)
    for p, kk in pairs:
        out_resid[p, kk] = -basis[0, p, kk]

    def apply_time(stage, half):
        arrived(*t_all, stage, half).wait_recv()
        to_spec(slopes[half] * time_of(stage, half), stage, half)

    def middle(stage):
        apply_time(stage, 0)
        halo_wait(stage)
        for p, kk in pairs:
            images[stage - 1, p, kk] = stencil(directions.at[stage - 1], stage, p, kk)
        apply_time(stage, 1)

    def finish_image(stage, half):
        part = halves[half]
        arrived(*l_all, stage, half).wait_recv()
        for p, kk in pairs:
            images[stage - 1, p, kk, part, :] = (
                images[stage - 1, p, kk, part, :] + spec_part(stage, half, p, kk)
            )

    def finish_and_send(stage):
        for half in range(2):
            finish_image(stage, half)
            precondition(images.at[stage - 1], directions.at[stage], half)
            to_time(directions.at[stage], stage + 1, half)
            exchange(*t_all, stage + 1, half)
        send_halo(directions.at[stage], stage + 1)

    middle(1)
    finish_and_send(1)

    reduce_start(0, [inner(p0, p0), inner(p0, i0), inner(i0, i0)])
    middle(2)
    reduce_middle(0)
    first = reduce_finish(0)
    h = first(1) / first(0)
    for p, kk in pairs:
        images[1, p, kk] = i1[p, kk] - h * i0[p, kk]
    finish_and_send(2)
    for p, kk in pairs:
        basis[1, p, kk] = i0[p, kk] - h * p0[p, kk]
        directions[1, p, kk] = z1[p, kk] - h * z0[p, kk]

    p1 = basis.at[1]
    reduce_start(
        1, [inner(p0, i1), inner(p1, i1), inner(p1, p1), inner(i0, i1), inner(i1, i1)]
    )
    middle(3)
    reduce_middle(1)
    second = reduce_finish(1)
    h0, h1 = second(0) / first(0), second(1) / second(2)
    for p, kk in pairs:
        images[2, p, kk] = i2[p, kk] - h0 * i0[p, kk] - h1 * i1[p, kk]
    finish_image(3, 0)
    finish_image(3, 1)
    reduce_start(2, [inner(p0, i2), inner(i0, i2), inner(i1, i2), inner(i2, i2)])
    for p, kk in pairs:
        directions[2, p, kk] = z2[p, kk] - h0 * z0[p, kk] - h1 * z1[p, kk]
    reduce_middle(2)
    third = reduce_finish(2)

    g00, g01, g02 = first(2), second(3), third(1)
    g11, g12, g22 = second(4), third(2), third(3)
    b0, b1, b2 = first(1), second(0), third(0)
    l10, l20 = g01 / g00, g02 / g00
    d1 = g11 - l10 * g01
    e12 = g12 - l10 * g02
    c1 = b1 - l10 * b0
    l21 = e12 / d1
    d2 = g22 - l20 * g02 - l21 * e12
    c2 = b2 - l20 * b0 - l21 * c1
    y2 = c2 / d2
    y1 = (c1 - e12 * y2) / d1
    y0 = (b0 - g01 * y1 - g02 * y2) / g00
    for p, kk in pairs:
        out_update[p, kk] = y0 * z0[p, kk] + y1 * z1[p, kk] + y2 * z2[p, kk]

    for stage in range(4):
        for half in range(2):
            arrived(*t_all, stage, half).wait_send()
            arrived(*l_all, stage, half).wait_send()
        for side in range(2):
            halo_copy(stage, side).wait_send()
    for stage in range(3):
        reduce_all(stage).wait_send()
        for d in range(3):
            ax_copy(stage, d).wait_send()


def body(state, source, capacity, row_shift, device_type, device_table, precond):
    inverse, forward = tables(state.shape[1] * lax.axis_size("harm"))
    block = (2, 2, 128, 128)
    vmem = pltpu.VMEM
    dma = pltpu.SemaphoreType.DMA
    hbm = pl.BlockSpec(memory_space=pltpu.HBM)
    update, resid = pl.pallas_call(
        kernel,
        out_shape=[jax.ShapeDtypeStruct(block, F32)] * 2,
        in_specs=[hbm] * 5 + [pl.BlockSpec(memory_space=pltpu.SMEM)] + [hbm] * 3,
        out_specs=[pl.BlockSpec(memory_space=vmem)] * 2,
        scratch_shapes=[
            vmem(block, F32), vmem(block, F32), vmem((128, 128), F32), vmem((1, 128), jnp.int32),
            vmem((128, 128), jnp.int32), vmem(block, F32), vmem((512, 256), BF16),
            vmem((512, 256), BF16),
            vmem((2, 256, 256), BF16), vmem((2, 256, 128), F32), vmem((2,) + block, F32),
            vmem((3,) + block, F32), vmem((3,) + block, F32),
            vmem((4, 2, 256, 128), F32), vmem((4, 2, 256, 128), F32),
            vmem((4, 2, 256, 128), F32), vmem((4, 2, 256, 128), F32),
            vmem((4, 2, 8, 128), F32), vmem((4, 2, 8, 128), F32),
            vmem((3, 1, 128), F32), vmem((3, 64, 1, 128), F32),
            vmem((3, 1, 128), F32), vmem((3, 4, 1, 128), F32),
            dma((8,)), dma((4, 2)), dma((4, 2)), dma((4, 2)), dma((4, 2)),
            dma((4, 2)), dma((4, 2)), dma((3,)), dma((3,)), dma((3, 3)), dma((3, 3)),
        ],
        compiler_params=pltpu.CompilerParams(
            collective_id=0, has_side_effects=True, vmem_limit_bytes=67_000_000
        ),
    )(
        state, source, capacity, row_shift.reshape(1, -1), device_type, device_table, precond,
        jnp.asarray(inverse), jnp.asarray(forward),
    )
    return update, resid


def solution(mesh):
    harm, node = mesh.axis_names
    return jax.shard_map(
        body,
        mesh=mesh,
        in_specs=(
            P(None, harm, node, None),
            P(None, harm, node, None),
            P(node, None),
            P(node),
            P(node, None),
            P(),
            P(None, harm, None, None),
        ),
        out_specs=(P(None, harm, node, None), P(None, harm, node, None)),
        check_vma=False,
    )
```

```python
import functools

import jax
import jax.numpy as jnp
import numpy as np
from jax import lax
from jax.experimental import pallas as pl
from jax.experimental.pallas import tpu as pltpu
from jax.sharding import PartitionSpec as P

ITERS = 3
TYPES = 4
SHIFTS = 4
FOLD = 1
OMEGA = 0.05
MESH = pl.DeviceIdType.MESH
F32 = jnp.float32
BF16 = jnp.bfloat16


def split(x):
    high = x.astype(BF16)
    low = (x - high.astype(F32)).astype(BF16)
    return high, low


def tables(harmonics):
    samples = 2 * harmonics
    row = np.arange(2 * harmonics)
    slot, q = row // 4, row % 4
    z_high, rest = slot % (8 // FOLD), slot // (8 // FOLD)
    z_low, y, core = rest // 8, rest // 2 % 4, rest % 2
    harm = y * 16 + (z_high * FOLD + z_low) * 2 + core
    wave, part = 2 * harm + q % 2, q // 2
    moment = np.arange(samples)
    phase = (moment[:, None] * wave[None, :] % samples) * (2.0 * np.pi / samples)
    inverse = np.where(part[None, :] == 0, np.cos(phase), -np.sin(phase))
    weight = np.where(wave == 0, 1.0, 2.0) / samples
    forward = inverse.T * weight[:, None]

    def stacked(matrix):
        matrix = matrix.astype(np.float32)
        high = matrix.astype(jnp.bfloat16)
        low = (matrix - high.astype(np.float32)).astype(jnp.bfloat16)
        return np.concatenate([high, low], axis=0)

    return stacked(inverse), stacked(forward)


def kernel(
    state_hbm, source_hbm, cap_hbm, shift_hbm, kinds_hbm, table, precond_hbm, inv_hbm, fwd_hbm,
    update_hbm, resid_hbm,
    state, source, cap, shift, kinds, precond, inv, fwd,
    gathered, weights, slopes, shifts, start, start_rows, first_z, direct, images,
    direct_back, out_update, out_resid,
    ta_send, ta_recv, la_send, la_recv, zf_recv, lg_send, lg_recv, tg_send, tg_recv,
    halo_send, halo_recv, ring_send, ring_recv, ar_send, ar_recv, ax_send, ax_recv,
    in_sem, out_sem, ta_ssem, ta_rsem, la_ssem, la_rsem, zf_ssem, zf_rsem, lg_ssem, lg_rsem, tg_ssem,
    tg_rsem, h_ssem, h_rsem, r_ssem, r_rsem, gz_ssem, gz_rsem, gx_ssem, gx_rsem, b_ssem, b_rsem,
    a_ssem, a_rsem, x_ssem, x_rsem,
):
    harm = lax.axis_index("harm")
    node = lax.axis_index("node")
    y, z, core = harm // 16, lax.rem(harm // 2, 8), lax.rem(harm, 2)
    chunks = 8 // FOLD
    group = 8 * FOLD
    zh, zl = z // FOLD, lax.rem(z, FOLD)
    mine = zl * 8 + y * 2 + core
    slot = mine * chunks + zh
    inputs = [
        (state_hbm, state), (precond_hbm, precond), (inv_hbm, inv), (kinds_hbm, kinds),
        (fwd_hbm, fwd), (shift_hbm, shift), (cap_hbm, cap), (source_hbm, source),
    ]
    loads = [pltpu.make_async_copy(a, b, in_sem.at[i]) for i, (a, b) in enumerate(inputs)]
    for load in loads:
        load.start()

    ys = [lax.rem(y + dy, 4) for dy in range(4)]
    cs = [lax.rem(core + dc, 2) for dc in range(2)]
    near = [(dy, dc) for dy in (2, 1, 3, 0) for dc in (1, 0)]

    def each_peer(act):
        @pl.loop(0, 7)
        def _(i):
            dz = jnp.where(lax.rem(i, 2) == 0, 4 + i // 2, 4 - (i + 1) // 2)
            other = lax.rem(z + dz, 8)
            base = other // FOLD + lax.rem(other, FOLD) * 8 * chunks
            for dy, dc in near:
                place = ys[dy] * 2 + cs[dc]
                act(ys[dy] * 16 + other * 2 + cs[dc], base + place * chunks)

        for dy, dc in near[:-1]:
            act(
                ys[dy] * 16 + z * 2 + cs[dc],
                zh + (zl * 8 + ys[dy] * 2 + cs[dc]) * chunks,
            )

    def each_mate(act):
        for dl in reversed(range(FOLD)):
            for dy, dc in near:
                if dl or dy or dc:
                    low = lax.rem(zl + dl, FOLD)
                    act(
                        ys[dy] * 16 + (zh * FOLD + low) * 2 + cs[dc],
                        low * 8 + ys[dy] * 2 + cs[dc],
                    )

    def along(d):
        high = lax.rem(zh + d, chunks)
        return y * 16 + (high * FOLD + zl) * 2 + core, high

    next_harm, prev_harm = along(1)[0], along(chunks - 1)[0]
    next_node = lax.rem(node + jnp.where(zh == chunks - 1, 1, 0), 4)
    prev_node = lax.rem(node + jnp.where(zh == 0, 3, 0), 4)
    ring = [(next_harm, next_node), (prev_harm, prev_node)]

    barrier = pltpu.get_barrier_semaphore()

    def greet(other, _):
        pl.semaphore_signal(barrier, inc=1, device_id=(other, node), device_id_type=MESH)

    each_peer(greet)
    for d in (1, 2, 3):
        pl.semaphore_signal(
            barrier, inc=1, device_id=(harm, lax.rem(node + d, 4)), device_id_type=MESH
        )
    for place in ring:
        pl.semaphore_signal(barrier, inc=1, device_id=place, device_id_type=MESH)

    def copy(src, dst, ssem, rsem, place):
        return pltpu.make_async_remote_copy(
            src_ref=src, dst_ref=dst, send_sem=ssem, recv_sem=rsem,
            device_id=place, device_id_type=MESH,
        )

    def unit(index):
        return pl.ds(pl.multiple_of(index * 4, 4), 4)

    def exchange(bufs, at):
        send, recv, ssem, rsem = bufs

        def push(other, other_slot):
            copy(
                send.at[*at, unit(other_slot)], recv.at[*at, unit(slot)],
                ssem.at[*at], rsem.at[*at], (other, node),
            ).start()

        each_peer(push)
        recv[*at, unit(slot), :] = send[*at, unit(slot), :]

    def exchanged(bufs, at):
        send, recv, ssem, rsem = bufs
        rows = pl.ds(0, 252)
        return copy(
            send.at[*at, rows], recv.at[*at, rows], ssem.at[*at], rsem.at[*at], (prev_harm, node)
        )

    wide = 4 * chunks

    def share(bufs, at):
        send, recv, ssem, rsem = bufs
        own = pl.ds(pl.multiple_of(mine * wide, wide), wide)

        def push(other, place):
            copy(
                send.at[*at, pl.ds(pl.multiple_of(place * wide, wide), wide)], recv.at[*at, own],
                ssem.at[*at], rsem.at[*at], (other, node),
            ).start()

        each_mate(push)
        recv[*at, own, :] = send[*at, own, :]

    def shared(bufs, at):
        send, recv, ssem, rsem = bufs
        rows = pl.ds(0, 256 - wide)
        return copy(
            send.at[*at, rows], recv.at[*at, rows],
            ssem.at[*at], rsem.at[*at], (prev_harm, node),
        )

    def spread(c, q):
        return pl.ds(c * 4 + q, group, stride=wide)

    ta = (ta_send, ta_recv, ta_ssem, ta_rsem)
    la = (la_send, la_recv, la_ssem, la_rsem)
    zf = (ta_recv.at[1], zf_recv, zf_ssem, zf_rsem)
    lg = (lg_send, lg_recv, lg_ssem, lg_rsem)
    tg = (tg_send, tg_recv, tg_ssem, tg_rsem)

    def halo_copy(side):
        step = 1 if side == 0 else 3
        return copy(
            halo_send.at[side], halo_recv.at[side], h_ssem.at[side], h_rsem.at[side],
            (harm, lax.rem(node + step, 4)),
        )

    def ring_copy(stage, side):
        return copy(
            ring_send.at[stage, side], ring_recv.at[stage, side],
            r_ssem.at[stage, side], r_rsem.at[stage, side], ring[side],
        )

    pairs = [(p, kk) for p in range(2) for kk in range(2)]
    deep = 2 * group

    def strip(chunk, half):
        return slice(chunk * deep + half * group, chunk * deep + (half + 1) * group)

    def to_time(field, stage, half):
        for p, kk in pairs:
            for c in range(chunks):
                ta_send[stage, half, spread(c, p * 2 + kk), :] = field[p, kk, strip(c, half), :]

    def product(matrix, x):
        high, low = split(x)
        all_parts = jnp.dot(
            matrix[...], jnp.concatenate([high, low], axis=1), preferred_element_type=F32
        )
        return (all_parts[0:256, 0:128] + all_parts[0:256, 128:256]) + all_parts[256:512, 0:128]

    loads[0].wait()
    to_time(state, 0, 0)
    loads[1].wait()
    for kk in range(2):
        gathered[zh, kk, :, 0:128] = precond[0, kk].T
        gathered[zh, kk, :, 128:256] = precond[1, kk].T

    def build(high_place):
        for kk in range(2):
            high, low = split(gathered[high_place, kk])
            weights[high_place, kk, 0:128, :] = high
            weights[high_place, kk, 128:256, :] = low

    build(zh)
    for load in loads[2:]:
        load.wait()
    params = []
    for half in range(2):
        kind = kinds[pl.ds(zh * deep + half * group + mine, 1), :]
        params.append(
            [
                sum(jnp.where(kind == member, table[what, member], 0.0) for member in range(TYPES))
                for what in range(3)
            ]
        )
    shifts[...] = jnp.broadcast_to(shift[...].astype(F32), (128, 128)).T

    pl.semaphore_wait(barrier, 68)
    exchange(ta, (0, 0))
    to_time(state, 0, 1)
    exchange(ta, (0, 1))
    last = [state[p, kk, 127:128, :] for p, kk in pairs]
    first = [state[p, kk, 0:1, :] for p, kk in pairs]
    halo_send[0] = jnp.concatenate(last + last, axis=0)
    halo_send[1] = jnp.concatenate(first + first, axis=0)
    for side in range(2):
        halo_copy(side).start()

    quarter = pl.ds(pl.multiple_of(node * 32, 32), 32)

    def along_z(way, step):
        high = along(step - 1 if way else chunks - (step - 1) if step > 1 else 0)[1]
        place = gathered.at[high, :, quarter]
        index = 4 * way + step - 1
        target = along(chunks - 1 if way else 1)[0]
        return copy(place, place, gz_ssem.at[index], gz_rsem.at[index], (target, node))

    def along_x(way, step, dx):
        high = along(step if way else chunks - step)[1]
        place = gathered.at[high, :, quarter]
        index = 4 * way + step - 1
        return copy(
            place, place, gx_ssem.at[index, dx - 1], gx_rsem.at[index, dx - 1],
            (harm, lax.rem(node + dx, 4)),
        )

    moves = [(way, step) for step in (1, 2, 3, 4) for way in (0, 1) if way == 0 or step < 4]

    def pass_on(step):
        for way, at in moves:
            if at == step:
                along_z(way, at).wait_recv()
        for way, at in moves:
            if at == step + 1:
                along_z(way, at).start()
        for dx in (2, 1, 3):
            for way, at in moves:
                if at == step:
                    along_x(way, at, dx).start()

    def receive(step):
        for way, at in moves:
            if at == step:
                for dx in (1, 2, 3):
                    along_x(way, at, dx).wait_recv()
                build(along(at if way else chunks - at)[1])

    for way, at in moves:
        if at == 1:
            along_z(way, at).start()

    def stencil(f, turned, halo_a, halo_b, shift_rows):
        rows = f.shape[0]
        row = lax.broadcasted_iota(jnp.int32, (rows, 128), 0)
        above = jnp.where(row == 0, halo_a, pltpu.roll(f, 1, axis=0))
        below = jnp.where(row == rows - 1, halo_b, pltpu.roll(f, rows - 1, axis=0))
        skewed = above
        for amount in range(1, SHIFTS):
            skewed = jnp.where(
                shift_rows == float(amount), pltpu.roll(above, 128 - amount, axis=1), skewed
            )
        sides = pltpu.roll(f, 1, axis=1) + pltpu.roll(f, 127, axis=1)
        return 4.0 * f - sides - skewed - below + turned

    zero = jnp.zeros((128, 128), BF16)

    def complex_product(u0, u1, weight):
        rows = u0.shape[0]
        high, low = split(jnp.concatenate([u0, u1], axis=0))
        left = jnp.concatenate(
            [
                jnp.concatenate([high, high], axis=1),
                jnp.concatenate([low, zero[0 : 2 * rows]], axis=1),
            ],
            axis=0,
        )
        out = jnp.dot(left, weight, preferred_element_type=F32)
        out = out[0 : 2 * rows] + out[2 * rows : 4 * rows]
        real = out[0:rows, 0:128] - out[rows : 2 * rows, 128:256]
        imag = out[0:rows, 128:256] + out[rows : 2 * rows, 0:128]
        return real, imag

    def evaluate(half):
        linear, amplitude, slope = params[half]
        exchanged(ta, (0, half)).wait_recv()
        voltage = product(inv, ta_recv[0, half])
        bent = jnp.tanh(slope * voltage)
        slopes[half] = linear + amplitude * slope * (1.0 - bent * bent)
        la_send[half] = product(fwd, linear * voltage + amplitude * bent)
        exchange(la, (half,))

    evaluate(0)
    for side in range(2):
        halo_copy(side).wait_recv()
    not_first = jnp.where(node == 0, 0.0, 1.0)
    not_last = jnp.where(node == 3, 0.0, 1.0)
    for p, kk in pairs:
        index = p * 2 + kk
        wave = (2 * harm + kk).astype(F32) * (-OMEGA if p == 0 else OMEGA)
        start[index] = source[p, kk] - stencil(
            state[p, kk],
            wave * cap[...] * state[1 - p, kk],
            halo_recv[0, index : index + 1, :] * not_first,
            halo_recv[1, index : index + 1, :] * not_last,
            shifts[...],
        )
    evaluate(1)
    pass_on(1)
    for half in range(2):
        exchanged(la, (half,)).wait_recv()
        for q in range(4):
            for c in range(chunks):
                part = strip(c, half)
                start[q, part, :] = start[q, part, :] - la_recv[half, spread(c, q), :]
        for kk in range(2):
            u0, u1 = [
                jnp.concatenate([start[q, strip(c, half), :] for c in range(chunks)], axis=0)
                for q in (kk, 2 + kk)
            ]
            real, imag = complex_product(u0, u1, weights[zh, kk])
            for q, value in ((kk, real), (2 + kk, imag)):
                for c in range(chunks):
                    piece = value[c * group : (c + 1) * group]
                    ta_send[1, half, spread(c, q), :] = piece
                    first_z[q, strip(c, half), :] = piece
        exchange(ta, (1, half))
        if half == 0:
            pass_on(2)
    receive(1)
    for p, kk in pairs:
        out_resid[p, kk] = -start[p * 2 + kk]
    resid_out = pltpu.make_async_copy(out_resid, resid_hbm, out_sem.at[4])
    resid_out.start()
    def to_spec(signal, stage, half):
        lg_send[stage, half] = product(fwd, signal)
        share(lg, (stage, half))

    for half in range(2):
        exchanged(ta, (1, half)).wait_recv()
        share(zf, (half,))
        to_spec(slopes[half] * product(inv, ta_recv[1, half]), 0, half)
        pass_on(3 + half)
    receive(2)

    def start_copy(d):
        other, high = along(d)
        return copy(
            start.at[:, pl.ds(pl.multiple_of(high * deep, deep), deep)], start_rows.at[zh],
            b_ssem.at[0, d - 1], b_rsem.at[0, d - 1], (other, node),
        )

    def back_copy(which, d):
        other, high = along(d)
        size = 4 * deep
        return copy(
            direct.at[which, pl.ds(pl.multiple_of(high * size, size), size)],
            direct_back.at[which - 1, pl.ds(pl.multiple_of(zh * size, size), size)],
            b_ssem.at[which, d - 1], b_rsem.at[which, d - 1], (other, node),
        )

    start_rows[zh] = start[:, pl.ds(pl.multiple_of(zh * deep, deep), deep), :]

    fields = [(c, q) for c in range(chunks) for q in range(4)]

    def at_rows(c, q, half=None):
        first_row = (c * 4 + q) * deep
        if half is None:
            return pl.ds(first_row, deep)
        return pl.ds(first_row + half * group, group)

    def send_ring(which):
        ring_send[which, 0] = direct[which, pl.ds(deep - 1, 4 * chunks, stride=deep), :]
        ring_send[which, 1] = direct[which, pl.ds(0, 4 * chunks, stride=deep), :]
        for side in range(2):
            ring_copy(which, side).start()

    chunk = pl.ds(pl.multiple_of(zh * deep, deep), deep)
    has_above = jnp.where((node == 0) & (zh == 0), 0.0, 1.0)
    has_below = jnp.where((node == 3) & (zh == chunks - 1), 0.0, 1.0)

    def local_image(which):
        for side in range(2):
            ring_copy(which, side).wait_recv()
        cap_rows, shift_rows = cap[chunk, :], shifts[chunk, :]
        for c, q in fields:
            p, kk = q // 2, q % 2
            place = y * 16 + (c * FOLD + zl) * 2 + core
            wave = (2 * place + kk).astype(F32) * (-OMEGA if p == 0 else OMEGA)
            index = c * 4 + q
            images[which, at_rows(c, q), :] = stencil(
                direct[which, at_rows(c, q), :],
                wave * cap_rows * direct[which, at_rows(c, (q + 2) % 4), :],
                ring_recv[which, 0, index : index + 1, :] * has_above,
                ring_recv[which, 1, index : index + 1, :] * has_below,
                shift_rows,
            )

    def finish_image(which, half):
        shared(lg, (which, half)).wait_recv()
        for c, q in fields:
            rows = at_rows(c, q, half)
            value = images[which, rows, :] + lg_recv[which, half, spread(c, q), :]
            if which > 0:
                value = value - images[which - 1, rows, :]
            images[which, rows, :] = value

    def send_direction(which, half):
        for c in range(chunks):
            for kk in range(2):
                real, imag = complex_product(
                    images[which - 1, at_rows(c, kk, half), :],
                    images[which - 1, at_rows(c, 2 + kk, half), :],
                    weights[c, kk],
                )
                for q, value in ((kk, real), (2 + kk, imag)):
                    direct[which, at_rows(c, q, half), :] = value
                    tg_send[which - 1, half, spread(c, q), :] = value
        share(tg, (which - 1, half))

    def inner(a, b, half):
        total = jnp.zeros((8, 128), F32)
        for c, q in fields:
            term = a(c, q, half) * b(c, q, half)
            for i in range(group // 8):
                total = total + term[i * 8 : (i + 1) * 8]
        return total

    def image_rows(which):
        return lambda c, q, half: images[which, at_rows(c, q, half), :]

    def start_part(c, q, half):
        return start_rows[c, q, half * group : (half + 1) * group, :]

    def closed(total):
        return jnp.sum(jnp.sum(total, axis=0, keepdims=True), axis=1, keepdims=True)

    for half in range(2):
        shared(zf, (half,)).wait_recv()
        for c, q in fields:
            direct[0, at_rows(c, q, half), :] = zf_recv[half, spread(c, q), :]
    send_ring(0)
    for d in range(1, chunks):
        start_copy(d).start()
    receive(3)
    receive(4)
    local_image(0)

    dots = {}
    for which in (1, 2):
        for half in range(2):
            finish_image(which - 1, half)
            send_direction(which, half)
        send_ring(which)
        for d in range(1, chunks):
            back_copy(which, d).start()
        size = 4 * deep
        own = pl.ds(pl.multiple_of(zh * size, size), size)
        direct_back[which - 1, own, :] = direct[which, own, :]
        for half in range(2):
            shared(tg, (which - 1, half)).wait_recv()
            to_spec(slopes[half] * product(inv, tg_recv[which - 1, half]), which, half)
        local_image(which)
        if which == 1:
            for d in range(1, chunks):
                start_copy(d).wait_recv()
        now = image_rows(which - 1)
        for name, other in [("start", start_part)] + [(j, image_rows(j)) for j in range(which)]:
            dots[name, which - 1] = closed(inner(other, now, 0) + inner(other, now, 1))
    others = [("start", start_part)] + [(j, image_rows(j)) for j in range(3)]
    sums = []
    for half in range(2):
        finish_image(2, half)
        sums.append([inner(other, image_rows(2), half) for _, other in others])
    for (name, _), one, two in zip(others, *sums):
        dots[name, 2] = closed(one + two)

    names = list(dots)
    lane = lax.broadcasted_iota(jnp.int32, (1, 128), 1)
    packed = sum(jnp.where(lane == i, dots[name], 0.0) for i, name in enumerate(names))
    ar_send[...] = packed

    def push(other, _):
        copy(ar_send, ar_recv.at[harm], a_ssem.at[0], a_rsem.at[0], (other, node)).start()

    each_peer(push)
    ar_recv[harm] = packed
    all_sums = copy(
        ar_recv.at[pl.ds(0, 63)], ar_recv.at[pl.ds(0, 63)], a_ssem.at[0], a_rsem.at[0],
        (prev_harm, node),
    )
    for half in range(2):
        for stage in range(2):
            exchanged(ta, (stage, half)).wait_send()
            shared(tg, (stage, half)).wait_send()
        exchanged(la, (half,)).wait_send()
        shared(zf, (half,)).wait_send()
        for stage in range(3):
            shared(lg, (stage, half)).wait_send()
    for side in range(2):
        halo_copy(side).wait_send()
        for stage in range(3):
            ring_copy(stage, side).wait_send()
    for d in range(1, chunks):
        start_copy(d).wait_send()
        for which in (1, 2):
            back_copy(which, d).wait_send()
    for way, at in moves:
        along_z(way, at).wait_send()
        for dx in (1, 2, 3):
            along_x(way, at, dx).wait_send()
    all_sums.wait_recv()
    total = jnp.sum(ar_recv[...], axis=0)
    ax_send[...] = total

    def ax_copy(dx):
        return copy(
            ax_send, ax_recv.at[node], x_ssem.at[dx - 1], x_rsem.at[dx - 1],
            (harm, lax.rem(node + dx, 4)),
        )

    for dx in (1, 2, 3):
        ax_copy(dx).start()
    ax_recv[node] = total
    for which in (1, 2):
        for d in range(1, chunks):
            back_copy(which, d).wait_recv()
    for dx in (1, 2, 3):
        ax_copy(dx).wait_recv()
    total = jnp.sum(ax_recv[...], axis=0)
    value = {name: total[:, i : i + 1] for i, name in enumerate(names)}

    g00, g01, g02 = value[0, 0], value[0, 1], value[0, 2]
    g11, g12, g22 = value[1, 1], value[1, 2], value[2, 2]
    b0, b1, b2 = value["start", 0], value["start", 1], value["start", 2]
    l10, l20 = g01 / g00, g02 / g00
    d1 = g11 - l10 * g01
    e12 = g12 - l10 * g02
    c1 = b1 - l10 * b0
    l21 = e12 / d1
    d2 = g22 - l20 * g02 - l21 * e12
    c2 = b2 - l20 * b0 - l21 * c1
    y2 = c2 / d2
    y1 = (c1 - e12 * y2) / d1
    y0 = (b0 - g01 * y1 - g02 * y2) / g00
    w0, w1, w2 = y0 - y1 + y2, y1 - y2, y2
    outs = [resid_out]
    for p, kk in pairs:
        q = p * 2 + kk
        for c in range(chunks):
            rows = slice(c * deep, (c + 1) * deep)
            out_update[p, kk, rows, :] = (
                w0 * first_z[q, rows, :]
                + w1 * direct_back[0, at_rows(c, q), :]
                + w2 * direct_back[1, at_rows(c, q), :]
            )
        outs.append(
            pltpu.make_async_copy(out_update.at[p, kk], update_hbm.at[p, kk], out_sem.at[q])
        )
        outs[-1].start()

    all_sums.wait_send()
    for dx in (1, 2, 3):
        ax_copy(dx).wait_send()
    for out in outs:
        out.wait()


def body(state, source, capacity, row_shift, device_type, device_table, precond):
    inverse, forward = tables(state.shape[1] * lax.axis_size("harm"))
    block = (2, 2, 128, 128)
    chunks, group = 8 // FOLD, 8 * FOLD
    vmem = pltpu.VMEM
    dma = pltpu.SemaphoreType.DMA
    hbm = pl.BlockSpec(memory_space=pltpu.HBM)

    def four(*lead):
        return [vmem(lead + (256, 128), F32)] * 2

    update, resid = pl.pallas_call(
        kernel,
        out_shape=[jax.ShapeDtypeStruct(block, F32)] * 2,
        in_specs=[hbm] * 5 + [pl.BlockSpec(memory_space=pltpu.SMEM)] + [hbm] * 3,
        out_specs=[hbm] * 2,
        scratch_shapes=[
            vmem(block, F32), vmem(block, F32), vmem((128, 128), F32), vmem((1, 128), jnp.int32),
            vmem((128, 128), jnp.int32), vmem(block, F32), vmem((512, 256), BF16),
            vmem((512, 256), BF16),
            vmem((chunks, 2, 128, 256), F32), vmem((chunks, 2, 256, 256), BF16),
            vmem((2, 256, 128), F32), vmem((128, 128), F32), vmem((4, 128, 128), F32),
            vmem((chunks, 4, 2 * group, 128), F32), vmem((4, 128, 128), F32),
            vmem((3, 512, 128), F32), vmem((3, 512, 128), F32), vmem((2, 512, 128), F32),
            vmem(block, F32), vmem(block, F32),
            *four(2, 2), *four(2), vmem((2, 256, 128), F32), *four(3, 2), *four(2, 2),
            vmem((2, 8, 128), F32), vmem((2, 8, 128), F32),
            vmem((3, 2, 4 * chunks, 128), F32), vmem((3, 2, 4 * chunks, 128), F32),
            vmem((1, 128), F32), vmem((64, 1, 128), F32),
            vmem((1, 128), F32), vmem((4, 1, 128), F32),
            dma((8,)), dma((5,)), dma((2, 2)), dma((2, 2)), dma((2,)), dma((2,)), dma((2,)), dma((2,)),
            dma((3, 2)), dma((3, 2)), dma((2, 2)), dma((2, 2)), dma((2,)), dma((2,)),
            dma((3, 2)), dma((3, 2)), dma((chunks - 1,)), dma((chunks - 1,)),
            dma((chunks - 1, 3)), dma((chunks - 1, 3)), dma((3, chunks - 1)),
            dma((3, chunks - 1)), dma((1,)), dma((1,)), dma((3,)), dma((3,)),
        ],
        compiler_params=pltpu.CompilerParams(
            collective_id=0, has_side_effects=True, vmem_limit_bytes=67_000_000
        ),
    )(
        state, source, capacity, row_shift.reshape(1, -1), device_type, device_table, precond,
        jnp.asarray(inverse), jnp.asarray(forward),
    )
    return update, resid


def solution(mesh):
    harm, node = mesh.axis_names
    return jax.shard_map(
        body,
        mesh=mesh,
        in_specs=(
            P(None, harm, node, None),
            P(None, harm, node, None),
            P(node, None),
            P(node),
            P(node, None),
            P(),
            P(None, harm, None, None),
        ),
        out_specs=(P(None, harm, node, None), P(None, harm, node, None)),
        check_vma=False,
    )
```

```python
import functools

import jax
import jax.numpy as jnp
import numpy as np
from jax import lax
from jax.experimental import pallas as pl
from jax.experimental.pallas import tpu as pltpu
from jax.sharding import PartitionSpec as P

ITERS = 3
TYPES = 4
SHIFTS = 4
FOLD = 1
OMEGA = 0.05
MESH = pl.DeviceIdType.MESH
F32 = jnp.float32
BF16 = jnp.bfloat16


def split(x):
    high = x.astype(BF16)
    low = (x - high.astype(F32)).astype(BF16)
    return high, low


def tables(harmonics):
    samples = 2 * harmonics
    row = np.arange(2 * harmonics)
    slot, q = row // 4, row % 4
    z_high, rest = slot % (8 // FOLD), slot // (8 // FOLD)
    z_low, y, core = rest // 8, rest // 2 % 4, rest % 2
    harm = y * 16 + (z_high * FOLD + z_low) * 2 + core
    wave, part = 2 * harm + q % 2, q // 2
    moment = np.arange(samples)
    phase = (moment[:, None] * wave[None, :] % samples) * (2.0 * np.pi / samples)
    inverse = np.where(part[None, :] == 0, np.cos(phase), -np.sin(phase))
    weight = np.where(wave == 0, 1.0, 2.0) / samples
    forward = inverse.T * weight[:, None]

    def stacked(matrix):
        matrix = matrix.astype(np.float32)
        high = matrix.astype(jnp.bfloat16)
        low = (matrix - high.astype(np.float32)).astype(jnp.bfloat16)
        return np.concatenate([high, low], axis=0)

    return stacked(inverse), stacked(forward)


def kernel(
    state_hbm, source_hbm, cap_hbm, shift_hbm, kinds_hbm, table, precond_hbm, inv_hbm, fwd_hbm,
    update_hbm, resid_hbm,
    state, source, cap, shift, kinds, precond, inv, fwd,
    gathered, weights, slopes, shifts, start, start_rows, first_z, direct, images,
    direct_back, out_update, out_resid,
    ta_send, ta_recv, la_send, la_recv, zf_recv, lg_send, lg_recv, tg_send, tg_recv,
    halo_send, halo_recv, ring_send, ring_recv, ar_send, ar_recv, ax_send, ax_recv,
    in_sem, out_sem, ta_ssem, ta_rsem, la_ssem, la_rsem, zf_ssem, zf_rsem, lg_ssem, lg_rsem, tg_ssem,
    tg_rsem, h_ssem, h_rsem, r_ssem, r_rsem, gz_ssem, gz_rsem, gx_ssem, gx_rsem, b_ssem, b_rsem,
    a_ssem, a_rsem, x_ssem, x_rsem,
):
    harm = lax.axis_index("harm")
    node = lax.axis_index("node")
    y, z, core = harm // 16, lax.rem(harm // 2, 8), lax.rem(harm, 2)
    chunks = 8 // FOLD
    group = 8 * FOLD
    zh, zl = z // FOLD, lax.rem(z, FOLD)
    mine = zl * 8 + y * 2 + core
    slot = mine * chunks + zh
    inputs = [
        (state_hbm, state), (precond_hbm, precond), (inv_hbm, inv), (kinds_hbm, kinds),
        (fwd_hbm, fwd), (shift_hbm, shift), (cap_hbm, cap), (source_hbm, source),
    ]
    loads = [pltpu.make_async_copy(a, b, in_sem.at[i]) for i, (a, b) in enumerate(inputs)]
    for load in loads:
        load.start()

    ys = [lax.rem(y + dy, 4) for dy in range(4)]
    cs = [lax.rem(core + dc, 2) for dc in range(2)]
    near = [(dy, dc) for dy in (2, 1, 3, 0) for dc in (1, 0)]

    def each_peer(act):
        @pl.loop(0, 7)
        def _(i):
            dz = jnp.where(lax.rem(i, 2) == 0, 4 + i // 2, 4 - (i + 1) // 2)
            other = lax.rem(z + dz, 8)
            base = other // FOLD + lax.rem(other, FOLD) * 8 * chunks
            for dy, dc in near:
                place = ys[dy] * 2 + cs[dc]
                act(ys[dy] * 16 + other * 2 + cs[dc], base + place * chunks)

        for dy, dc in near[:-1]:
            act(
                ys[dy] * 16 + z * 2 + cs[dc],
                zh + (zl * 8 + ys[dy] * 2 + cs[dc]) * chunks,
            )

    def each_mate(act):
        for dl in reversed(range(FOLD)):
            for dy, dc in near:
                if dl or dy or dc:
                    low = lax.rem(zl + dl, FOLD)
                    act(
                        ys[dy] * 16 + (zh * FOLD + low) * 2 + cs[dc],
                        low * 8 + ys[dy] * 2 + cs[dc],
                    )

    def along(d):
        high = lax.rem(zh + d, chunks)
        return y * 16 + (high * FOLD + zl) * 2 + core, high

    next_harm, prev_harm = along(1)[0], along(chunks - 1)[0]
    next_node = lax.rem(node + jnp.where(zh == chunks - 1, 1, 0), 4)
    prev_node = lax.rem(node + jnp.where(zh == 0, 3, 0), 4)
    ring = [(next_harm, next_node), (prev_harm, prev_node)]

    barrier = pltpu.get_barrier_semaphore()

    def greet(other, _):
        pl.semaphore_signal(barrier, inc=1, device_id=(other, node), device_id_type=MESH)

    each_peer(greet)
    for d in (1, 2, 3):
        pl.semaphore_signal(
            barrier, inc=1, device_id=(harm, lax.rem(node + d, 4)), device_id_type=MESH
        )
    for place in ring:
        pl.semaphore_signal(barrier, inc=1, device_id=place, device_id_type=MESH)

    def copy(src, dst, ssem, rsem, place):
        return pltpu.make_async_remote_copy(
            src_ref=src, dst_ref=dst, send_sem=ssem, recv_sem=rsem,
            device_id=place, device_id_type=MESH,
        )

    def unit(index):
        return pl.ds(pl.multiple_of(index * 4, 4), 4)

    def exchange(bufs, at):
        send, recv, ssem, rsem = bufs

        def push(other, other_slot):
            copy(
                send.at[*at, unit(other_slot)], recv.at[*at, unit(slot)],
                ssem.at[0], rsem.at[*at], (other, node),
            ).start()

        each_peer(push)
        recv[*at, unit(slot), :] = send[*at, unit(slot), :]

    def exchanged(bufs, at):
        send, recv, ssem, rsem = bufs
        rows = pl.ds(0, 252)
        return copy(
            send.at[*at, rows], recv.at[*at, rows], ssem.at[0], rsem.at[*at], (prev_harm, node)
        )

    wide = 4 * chunks

    def share(bufs, at):
        send, recv, ssem, rsem = bufs
        own = pl.ds(pl.multiple_of(mine * wide, wide), wide)

        def push(other, place):
            copy(
                send.at[*at, pl.ds(pl.multiple_of(place * wide, wide), wide)], recv.at[*at, own],
                ssem.at[0], rsem.at[*at], (other, node),
            ).start()

        each_mate(push)
        recv[*at, own, :] = send[*at, own, :]

    def shared(bufs, at):
        send, recv, ssem, rsem = bufs
        rows = pl.ds(0, 256 - wide)
        return copy(
            send.at[*at, rows], recv.at[*at, rows],
            ssem.at[0], rsem.at[*at], (prev_harm, node),
        )

    def spread(c, q):
        return pl.ds(c * 4 + q, group, stride=wide)

    ta = (ta_send, ta_recv, ta_ssem, ta_rsem)
    la = (la_send, la_recv, la_ssem, la_rsem)
    zf = (ta_recv.at[1], zf_recv, zf_ssem, zf_rsem)
    lg = (lg_send, lg_recv, lg_ssem, lg_rsem)
    tg = (tg_send, tg_recv, tg_ssem, tg_rsem)

    def halo_copy(side):
        step = 1 if side == 0 else 3
        return copy(
            halo_send.at[side], halo_recv.at[side], h_ssem.at[0], h_rsem.at[0],
            (harm, lax.rem(node + step, 4)),
        )

    halo_both = copy(halo_send, halo_recv, h_ssem.at[0], h_rsem.at[0], ring[0])

    def ring_copy(stage, side):
        return copy(
            ring_send.at[stage, side], ring_recv.at[stage, side],
            r_ssem.at[0], r_rsem.at[stage], ring[side],
        )

    def ring_both(stage):
        return copy(
            ring_send.at[stage], ring_recv.at[stage], r_ssem.at[0], r_rsem.at[stage], ring[0]
        )

    pairs = [(p, kk) for p in range(2) for kk in range(2)]
    deep = 2 * group

    def strip(chunk, half):
        return slice(chunk * deep + half * group, chunk * deep + (half + 1) * group)

    def to_time(field, stage, half):
        for p, kk in pairs:
            for c in range(chunks):
                ta_send[stage, half, spread(c, p * 2 + kk), :] = field[p, kk, strip(c, half), :]

    def product(matrix, x):
        high, low = split(x)
        all_parts = jnp.dot(
            matrix[...], jnp.concatenate([high, low], axis=1), preferred_element_type=F32
        )
        return (all_parts[0:256, 0:128] + all_parts[0:256, 128:256]) + all_parts[256:512, 0:128]

    loads[0].wait()
    to_time(state, 0, 0)
    loads[1].wait()
    for kk in range(2):
        gathered[zh, kk, :, 0:128] = precond[0, kk].T
        gathered[zh, kk, :, 128:256] = precond[1, kk].T

    def build(high_place):
        for kk in range(2):
            high, low = split(gathered[high_place, kk])
            weights[high_place, kk, 0:128, :] = high
            weights[high_place, kk, 128:256, :] = low

    build(zh)
    for load in loads[2:]:
        load.wait()
    params = []
    for half in range(2):
        kind = kinds[pl.ds(zh * deep + half * group + mine, 1), :]
        params.append(
            [
                sum(jnp.where(kind == member, table[what, member], 0.0) for member in range(TYPES))
                for what in range(3)
            ]
        )
    shifts[...] = jnp.broadcast_to(shift[...].astype(F32), (128, 128)).T

    pl.semaphore_wait(barrier, 68)
    exchange(ta, (0, 0))
    to_time(state, 0, 1)
    exchange(ta, (0, 1))
    last = [state[p, kk, 127:128, :] for p, kk in pairs]
    first = [state[p, kk, 0:1, :] for p, kk in pairs]
    halo_send[0] = jnp.concatenate(last + last, axis=0)
    halo_send[1] = jnp.concatenate(first + first, axis=0)
    for side in range(2):
        halo_copy(side).start()

    quarter = pl.ds(pl.multiple_of(node * 32, 32), 32)

    def along_z(way, step):
        high = along(step - 1 if way else chunks - (step - 1) if step > 1 else 0)[1]
        place = gathered.at[high, :, quarter]
        target = along(chunks - 1 if way else 1)[0]
        return copy(place, place, gz_ssem.at[0], gz_rsem.at[step - 1], (target, node))

    def along_x(way, step, dx):
        high = along(step if way else chunks - step)[1]
        place = gathered.at[high, :, quarter]
        return copy(
            place, place, gx_ssem.at[0], gx_rsem.at[step - 1], (harm, lax.rem(node + dx, 4))
        )

    def bulk(count, rows, ssem, rsem):
        place = gathered.at[pl.ds(0, count), :, pl.ds(0, rows)]
        return copy(place, place, ssem, rsem, (prev_harm, node))

    moves = [(way, step) for step in (1, 2, 3, 4) for way in (0, 1) if way == 0 or step < 4]

    def pass_on(step):
        ways = 2 if step < 4 else 1
        bulk(ways, 32, gz_ssem.at[0], gz_rsem.at[step - 1]).wait_recv()
        for way, at in moves:
            if at == step + 1:
                along_z(way, at).start()
        for dx in (2, 1, 3):
            for way, at in moves:
                if at == step:
                    along_x(way, at, dx).start()

    def receive(step):
        ways = 2 if step < 4 else 1
        bulk(ways, 96, gx_ssem.at[0], gx_rsem.at[step - 1]).wait_recv()
        for way, at in moves:
            if at == step:
                build(along(at if way else chunks - at)[1])

    for way, at in moves:
        if at == 1:
            along_z(way, at).start()

    def stencil(f, turned, halo_a, halo_b, shift_rows):
        rows = f.shape[0]
        row = lax.broadcasted_iota(jnp.int32, (rows, 128), 0)
        above = jnp.where(row == 0, halo_a, pltpu.roll(f, 1, axis=0))
        below = jnp.where(row == rows - 1, halo_b, pltpu.roll(f, rows - 1, axis=0))
        skewed = above
        for amount in range(1, SHIFTS):
            skewed = jnp.where(
                shift_rows == float(amount), pltpu.roll(above, 128 - amount, axis=1), skewed
            )
        sides = pltpu.roll(f, 1, axis=1) + pltpu.roll(f, 127, axis=1)
        return 4.0 * f - sides - skewed - below + turned

    zero = jnp.zeros((128, 128), BF16)

    def complex_product(u0, u1, weight):
        rows = u0.shape[0]
        high, low = split(jnp.concatenate([u0, u1], axis=0))
        left = jnp.concatenate(
            [
                jnp.concatenate([high, high], axis=1),
                jnp.concatenate([low, zero[0 : 2 * rows]], axis=1),
            ],
            axis=0,
        )
        out = jnp.dot(left, weight, preferred_element_type=F32)
        out = out[0 : 2 * rows] + out[2 * rows : 4 * rows]
        real = out[0:rows, 0:128] - out[rows : 2 * rows, 128:256]
        imag = out[0:rows, 128:256] + out[rows : 2 * rows, 0:128]
        return real, imag

    def evaluate(half):
        linear, amplitude, slope = params[half]
        exchanged(ta, (0, half)).wait_recv()
        voltage = product(inv, ta_recv[0, half])
        bent = jnp.tanh(slope * voltage)
        slopes[half] = linear + amplitude * slope * (1.0 - bent * bent)
        la_send[half] = product(fwd, linear * voltage + amplitude * bent)
        exchange(la, (half,))

    evaluate(0)
    halo_both.wait_recv()
    not_first = jnp.where(node == 0, 0.0, 1.0)
    not_last = jnp.where(node == 3, 0.0, 1.0)
    for p, kk in pairs:
        index = p * 2 + kk
        wave = (2 * harm + kk).astype(F32) * (-OMEGA if p == 0 else OMEGA)
        start[index] = source[p, kk] - stencil(
            state[p, kk],
            wave * cap[...] * state[1 - p, kk],
            halo_recv[0, index : index + 1, :] * not_first,
            halo_recv[1, index : index + 1, :] * not_last,
            shifts[...],
        )
    evaluate(1)
    pass_on(1)
    for half in range(2):
        exchanged(la, (half,)).wait_recv()
        for q in range(4):
            for c in range(chunks):
                part = strip(c, half)
                start[q, part, :] = start[q, part, :] - la_recv[half, spread(c, q), :]
        for kk in range(2):
            u0, u1 = [
                jnp.concatenate([start[q, strip(c, half), :] for c in range(chunks)], axis=0)
                for q in (kk, 2 + kk)
            ]
            real, imag = complex_product(u0, u1, weights[zh, kk])
            for q, value in ((kk, real), (2 + kk, imag)):
                for c in range(chunks):
                    piece = value[c * group : (c + 1) * group]
                    ta_send[1, half, spread(c, q), :] = piece
                    first_z[q, strip(c, half), :] = piece
        exchange(ta, (1, half))
        if half == 0:
            pass_on(2)
    receive(1)
    for p, kk in pairs:
        out_resid[p, kk] = -start[p * 2 + kk]
    resid_out = pltpu.make_async_copy(out_resid, resid_hbm, out_sem.at[1])
    resid_out.start()
    def to_spec(signal, stage, half):
        lg_send[stage, half] = product(fwd, signal)
        share(lg, (stage, half))

    for half in range(2):
        exchanged(ta, (1, half)).wait_recv()
        share(zf, (half,))
        to_spec(slopes[half] * product(inv, ta_recv[1, half]), 0, half)
        pass_on(3 + half)
    receive(2)

    def start_copy(d):
        other, high = along(d)
        return copy(
            start.at[:, pl.ds(pl.multiple_of(high * deep, deep), deep)], start_rows.at[zh],
            b_ssem.at[0], b_rsem.at[0], (other, node),
        )

    def back_copy(which, d):
        other, high = along(d)
        size = 4 * deep
        return copy(
            direct.at[which, pl.ds(pl.multiple_of(high * size, size), size)],
            direct_back.at[which - 1, pl.ds(pl.multiple_of(zh * size, size), size)],
            b_ssem.at[1], b_rsem.at[1], (other, node),
        )

    start_rows[zh] = start[:, pl.ds(pl.multiple_of(zh * deep, deep), deep), :]

    rows_of_others = start_rows.at[pl.ds(0, chunks - 1)]
    start_all = copy(
        rows_of_others, rows_of_others, b_ssem.at[0], b_rsem.at[0], (prev_harm, node)
    )
    back_of_others = direct_back.at[:, pl.ds(0, 512 - 4 * deep)]
    back_all = copy(
        back_of_others, back_of_others, b_ssem.at[1], b_rsem.at[1], (prev_harm, node)
    )

    fields = [(c, q) for c in range(chunks) for q in range(4)]

    def at_rows(c, q, half=None):
        first_row = (c * 4 + q) * deep
        if half is None:
            return pl.ds(first_row, deep)
        return pl.ds(first_row + half * group, group)

    def send_ring(which):
        ring_send[which, 0] = direct[which, pl.ds(deep - 1, 4 * chunks, stride=deep), :]
        ring_send[which, 1] = direct[which, pl.ds(0, 4 * chunks, stride=deep), :]
        for side in range(2):
            ring_copy(which, side).start()

    chunk = pl.ds(pl.multiple_of(zh * deep, deep), deep)
    has_above = jnp.where((node == 0) & (zh == 0), 0.0, 1.0)
    has_below = jnp.where((node == 3) & (zh == chunks - 1), 0.0, 1.0)

    def local_image(which):
        ring_both(which).wait_recv()
        cap_rows, shift_rows = cap[chunk, :], shifts[chunk, :]
        for c, q in fields:
            p, kk = q // 2, q % 2
            place = y * 16 + (c * FOLD + zl) * 2 + core
            wave = (2 * place + kk).astype(F32) * (-OMEGA if p == 0 else OMEGA)
            index = c * 4 + q
            images[which, at_rows(c, q), :] = stencil(
                direct[which, at_rows(c, q), :],
                wave * cap_rows * direct[which, at_rows(c, (q + 2) % 4), :],
                ring_recv[which, 0, index : index + 1, :] * has_above,
                ring_recv[which, 1, index : index + 1, :] * has_below,
                shift_rows,
            )

    def finish_image(which, half):
        shared(lg, (which, half)).wait_recv()
        for c, q in fields:
            rows = at_rows(c, q, half)
            value = images[which, rows, :] + lg_recv[which, half, spread(c, q), :]
            if which > 0:
                value = value - images[which - 1, rows, :]
            images[which, rows, :] = value

    def send_direction(which, half):
        for c in range(chunks):
            for kk in range(2):
                real, imag = complex_product(
                    images[which - 1, at_rows(c, kk, half), :],
                    images[which - 1, at_rows(c, 2 + kk, half), :],
                    weights[c, kk],
                )
                for q, value in ((kk, real), (2 + kk, imag)):
                    direct[which, at_rows(c, q, half), :] = value
                    tg_send[which - 1, half, spread(c, q), :] = value
        share(tg, (which - 1, half))

    def inner(a, b, half):
        total = jnp.zeros((8, 128), F32)
        for c, q in fields:
            term = a(c, q, half) * b(c, q, half)
            for i in range(group // 8):
                total = total + term[i * 8 : (i + 1) * 8]
        return total

    def image_rows(which):
        return lambda c, q, half: images[which, at_rows(c, q, half), :]

    def start_part(c, q, half):
        return start_rows[c, q, half * group : (half + 1) * group, :]

    def closed(total):
        return jnp.sum(jnp.sum(total, axis=0, keepdims=True), axis=1, keepdims=True)

    for half in range(2):
        shared(zf, (half,)).wait_recv()
        for c, q in fields:
            direct[0, at_rows(c, q, half), :] = zf_recv[half, spread(c, q), :]
    send_ring(0)
    for d in range(1, chunks):
        start_copy(d).start()
    receive(3)
    receive(4)
    local_image(0)

    dots = {}
    for which in (1, 2):
        for half in range(2):
            finish_image(which - 1, half)
            send_direction(which, half)
        send_ring(which)
        for d in range(1, chunks):
            back_copy(which, d).start()
        size = 4 * deep
        own = pl.ds(pl.multiple_of(zh * size, size), size)
        direct_back[which - 1, own, :] = direct[which, own, :]
        for half in range(2):
            shared(tg, (which - 1, half)).wait_recv()
            to_spec(slopes[half] * product(inv, tg_recv[which - 1, half]), which, half)
        local_image(which)
        if which == 1:
            start_all.wait_recv()
        now = image_rows(which - 1)
        for name, other in [("start", start_part)] + [(j, image_rows(j)) for j in range(which)]:
            dots[name, which - 1] = closed(inner(other, now, 0) + inner(other, now, 1))
    others = [("start", start_part)] + [(j, image_rows(j)) for j in range(3)]
    sums = []
    for half in range(2):
        finish_image(2, half)
        sums.append([inner(other, image_rows(2), half) for _, other in others])
    for (name, _), one, two in zip(others, *sums):
        dots[name, 2] = closed(one + two)

    names = list(dots)
    lane = lax.broadcasted_iota(jnp.int32, (1, 128), 1)
    packed = sum(jnp.where(lane == i, dots[name], 0.0) for i, name in enumerate(names))
    ar_send[...] = packed

    def push(other, _):
        copy(ar_send, ar_recv.at[harm], a_ssem.at[0], a_rsem.at[0], (other, node)).start()

    each_peer(push)
    ar_recv[harm] = packed
    all_sums = copy(
        ar_recv.at[pl.ds(0, 63)], ar_recv.at[pl.ds(0, 63)], a_ssem.at[0], a_rsem.at[0],
        (prev_harm, node),
    )
    def left(part, ssem):
        copy(part, part, ssem, a_rsem.at[0], (prev_harm, node)).wait_send()

    left(ta_send.at[:, :, pl.ds(0, 252)], ta_ssem.at[0])
    left(la_send.at[:, pl.ds(0, 252)], la_ssem.at[0])
    left(zf_recv.at[:, pl.ds(0, 256 - wide)], zf_ssem.at[0])
    left(lg_send.at[:, :, pl.ds(0, 256 - wide)], lg_ssem.at[0])
    left(tg_send.at[:, :, pl.ds(0, 256 - wide)], tg_ssem.at[0])
    left(ring_send, r_ssem.at[0])
    halo_both.wait_send()
    bulk(7, 32, gz_ssem.at[0], gz_rsem.at[0]).wait_send()
    bulk(7, 96, gx_ssem.at[0], gx_rsem.at[0]).wait_send()
    start_all.wait_send()
    back_all.wait_send()
    all_sums.wait_recv()
    total = jnp.sum(ar_recv[...], axis=0)
    ax_send[...] = total

    def ax_copy(dx):
        return copy(
            ax_send, ax_recv.at[node], x_ssem.at[0], x_rsem.at[0],
            (harm, lax.rem(node + dx, 4)),
        )

    for dx in (1, 2, 3):
        ax_copy(dx).start()
    ax_recv[node] = total
    back_all.wait_recv()
    ax_all = copy(
        ax_recv.at[pl.ds(0, 3)], ax_recv.at[pl.ds(0, 3)], x_ssem.at[0], x_rsem.at[0], ring[0]
    )
    ax_all.wait_recv()
    total = jnp.sum(ax_recv[...], axis=0)
    value = {name: total[:, i : i + 1] for i, name in enumerate(names)}

    g00, g01, g02 = value[0, 0], value[0, 1], value[0, 2]
    g11, g12, g22 = value[1, 1], value[1, 2], value[2, 2]
    b0, b1, b2 = value["start", 0], value["start", 1], value["start", 2]
    l10, l20 = g01 / g00, g02 / g00
    d1 = g11 - l10 * g01
    e12 = g12 - l10 * g02
    c1 = b1 - l10 * b0
    l21 = e12 / d1
    d2 = g22 - l20 * g02 - l21 * e12
    c2 = b2 - l20 * b0 - l21 * c1
    y2 = c2 / d2
    y1 = (c1 - e12 * y2) / d1
    y0 = (b0 - g01 * y1 - g02 * y2) / g00
    w0, w1, w2 = y0 - y1 + y2, y1 - y2, y2
    for p, kk in pairs:
        q = p * 2 + kk
        for c in range(chunks):
            rows = slice(c * deep, (c + 1) * deep)
            out_update[p, kk, rows, :] = (
                w0 * first_z[q, rows, :]
                + w1 * direct_back[0, at_rows(c, q), :]
                + w2 * direct_back[1, at_rows(c, q), :]
            )
        pltpu.make_async_copy(out_update.at[p, kk], update_hbm.at[p, kk], out_sem.at[0]).start()

    all_sums.wait_send()
    ax_all.wait_send()
    pltpu.make_async_copy(out_update, update_hbm, out_sem.at[0]).wait()
    resid_out.wait()


def hand_over(update, resid, update_out, resid_out, held, in_sem, out_sem):
    ways = [(update, update_out), (resid, resid_out)]
    loads = [pltpu.make_async_copy(a, held.at[i], in_sem.at[i]) for i, (a, _) in enumerate(ways)]
    stores = [pltpu.make_async_copy(held.at[i], b, out_sem.at[i]) for i, (_, b) in enumerate(ways)]
    for load in loads:
        load.start()
    for load, store in zip(loads, stores):
        load.wait()
        store.start()
    for store in stores:
        store.wait()


def body(state, source, capacity, row_shift, device_type, device_table, precond):
    inverse, forward = tables(state.shape[1] * lax.axis_size("harm"))
    block = (2, 2, 128, 128)
    chunks, group = 8 // FOLD, 8 * FOLD
    vmem = pltpu.VMEM
    dma = pltpu.SemaphoreType.DMA
    hbm = pl.BlockSpec(memory_space=pltpu.HBM)

    def four(*lead):
        return [vmem(lead + (256, 128), F32)] * 2

    update, resid = pl.pallas_call(
        kernel,
        out_shape=[jax.ShapeDtypeStruct(block, F32)] * 2,
        in_specs=[hbm] * 5 + [pl.BlockSpec(memory_space=pltpu.SMEM)] + [hbm] * 3,
        out_specs=[hbm] * 2,
        scratch_shapes=[
            vmem(block, F32), vmem(block, F32), vmem((128, 128), F32), vmem((1, 128), jnp.int32),
            vmem((128, 128), jnp.int32), vmem(block, F32), vmem((512, 256), BF16),
            vmem((512, 256), BF16),
            vmem((chunks, 2, 128, 256), F32), vmem((chunks, 2, 256, 256), BF16),
            vmem((2, 256, 128), F32), vmem((128, 128), F32), vmem((4, 128, 128), F32),
            vmem((chunks, 4, 2 * group, 128), F32), vmem((4, 128, 128), F32),
            vmem((3, 512, 128), F32), vmem((3, 512, 128), F32), vmem((2, 512, 128), F32),
            vmem(block, F32), vmem(block, F32),
            *four(2, 2), *four(2), vmem((2, 256, 128), F32), *four(3, 2), *four(2, 2),
            vmem((2, 8, 128), F32), vmem((2, 8, 128), F32),
            vmem((3, 2, 4 * chunks, 128), F32), vmem((3, 2, 4 * chunks, 128), F32),
            vmem((1, 128), F32), vmem((64, 1, 128), F32),
            vmem((1, 128), F32), vmem((4, 1, 128), F32),
            dma((8,)), dma((2,)), dma((1,)), dma((2, 2)), dma((1,)), dma((2,)), dma((1,)),
            dma((2,)), dma((1,)), dma((3, 2)), dma((1,)), dma((2, 2)), dma((1,)), dma((1,)),
            dma((1,)), dma((3,)), dma((1,)), dma((4,)), dma((1,)), dma((4,)), dma((2,)),
            dma((2,)), dma((1,)), dma((1,)), dma((1,)), dma((1,)),
        ],
        compiler_params=pltpu.CompilerParams(
            collective_id=0, has_side_effects=True, vmem_limit_bytes=67_000_000
        ),
    )(
        state, source, capacity, row_shift.reshape(1, -1), device_type, device_table, precond,
        jnp.asarray(inverse), jnp.asarray(forward),
    )
    return pl.pallas_call(
        hand_over,
        out_shape=[jax.ShapeDtypeStruct(block, F32)] * 2,
        in_specs=[hbm] * 2,
        out_specs=[hbm] * 2,
        scratch_shapes=[vmem((2,) + block, F32), dma((2,)), dma((2,))],
        compiler_params=pltpu.CompilerParams(vmem_limit_bytes=67_000_000),
    )(update, resid)


def solution(mesh):
    harm, node = mesh.axis_names
    return jax.shard_map(
        body,
        mesh=mesh,
        in_specs=(
            P(None, harm, node, None),
            P(None, harm, node, None),
            P(node, None),
            P(node),
            P(node, None),
            P(),
            P(None, harm, None, None),
        ),
        out_specs=(P(None, harm, node, None), P(None, harm, node, None)),
        check_vma=False,
    )
```

```python
import functools

import jax
import jax.numpy as jnp
import numpy as np
from jax import lax
from jax.experimental import pallas as pl
from jax.experimental.pallas import tpu as pltpu
from jax.sharding import PartitionSpec as P

ITERS = 3
TYPES = 4
SHIFTS = 4
FOLD = 1
OMEGA = 0.05
MESH = pl.DeviceIdType.MESH
F32 = jnp.float32
BF16 = jnp.bfloat16


def split(x):
    high = x.astype(BF16)
    low = (x - high.astype(F32)).astype(BF16)
    return high, low


def tables(harmonics):
    samples = 2 * harmonics
    row = np.arange(2 * harmonics)
    slot, q = row // 4, row % 4
    z_high, rest = slot % (8 // FOLD), slot // (8 // FOLD)
    z_low, y, core = rest // 8, rest // 2 % 4, rest % 2
    harm = y * 16 + (z_high * FOLD + z_low) * 2 + core
    wave, part = 2 * harm + q % 2, q // 2
    moment = np.arange(samples)
    phase = (moment[:, None] * wave[None, :] % samples) * (2.0 * np.pi / samples)
    inverse = np.where(part[None, :] == 0, np.cos(phase), -np.sin(phase))
    weight = np.where(wave == 0, 1.0, 2.0) / samples
    forward = inverse.T * weight[:, None]

    def stacked(matrix):
        matrix = matrix.astype(np.float32)
        high = matrix.astype(jnp.bfloat16)
        low = (matrix - high.astype(np.float32)).astype(jnp.bfloat16)
        return np.concatenate([high, low], axis=0)

    return stacked(inverse), stacked(forward)


def kernel(
    state_hbm, source_hbm, cap_hbm, shift_hbm, kinds_hbm, table, precond_hbm, inv_hbm, fwd_hbm,
    update_hbm, resid_hbm,
    state, source, cap, shift, kinds, precond, inv, fwd,
    gathered, weights, slopes, shifts, start, start_rows, first_z, direct, images,
    direct_back, out_update, out_resid,
    ta_send, ta_recv, la_send, la_recv, zf_recv, lg_send, lg_recv, tg_send, tg_recv,
    halo_send, halo_recv, ring_send, ring_recv, ar_send, ar_recv, ax_send, ax_recv,
    in_sem, out_sem, ta_ssem, ta_rsem, la_ssem, la_rsem, zf_ssem, zf_rsem, lg_ssem, lg_rsem, tg_ssem,
    tg_rsem, h_ssem, h_rsem, r_ssem, r_rsem, gz_ssem, gz_rsem, gx_ssem, gx_rsem, b_ssem, b_rsem,
    a_ssem, a_rsem, x_ssem, x_rsem,
):
    harm = lax.axis_index("harm")
    node = lax.axis_index("node")
    y, z, core = harm // 16, lax.rem(harm // 2, 8), lax.rem(harm, 2)
    chunks = 8 // FOLD
    group = 8 * FOLD
    zh, zl = z // FOLD, lax.rem(z, FOLD)
    mine = zl * 8 + y * 2 + core
    slot = mine * chunks + zh
    inputs = [
        (state_hbm, state), (precond_hbm, precond), (inv_hbm, inv), (kinds_hbm, kinds),
        (fwd_hbm, fwd), (shift_hbm, shift), (cap_hbm, cap), (source_hbm, source),
    ]
    loads = [pltpu.make_async_copy(a, b, in_sem.at[i]) for i, (a, b) in enumerate(inputs)]
    for load in loads:
        load.start()

    ys = [lax.rem(y + dy, 4) for dy in range(4)]
    cs = [lax.rem(core + dc, 2) for dc in range(2)]
    near = [(dy, dc) for dy in (2, 1, 3, 0) for dc in (1, 0)]

    def each_peer(act):
        @pl.loop(0, 7)
        def _(i):
            dz = jnp.where(lax.rem(i, 2) == 0, 4 + i // 2, 4 - (i + 1) // 2)
            other = lax.rem(z + dz, 8)
            base = other // FOLD + lax.rem(other, FOLD) * 8 * chunks
            for dy, dc in near:
                place = ys[dy] * 2 + cs[dc]
                act(ys[dy] * 16 + other * 2 + cs[dc], base + place * chunks)

        for dy, dc in near[:-1]:
            act(
                ys[dy] * 16 + z * 2 + cs[dc],
                zh + (zl * 8 + ys[dy] * 2 + cs[dc]) * chunks,
            )

    def each_mate(act):
        for dl in reversed(range(FOLD)):
            for dy, dc in near:
                if dl or dy or dc:
                    low = lax.rem(zl + dl, FOLD)
                    act(
                        ys[dy] * 16 + (zh * FOLD + low) * 2 + cs[dc],
                        low * 8 + ys[dy] * 2 + cs[dc],
                    )

    def along(d):
        high = lax.rem(zh + d, chunks)
        return y * 16 + (high * FOLD + zl) * 2 + core, high

    next_harm, prev_harm = along(1)[0], along(chunks - 1)[0]
    next_node = lax.rem(node + jnp.where(zh == chunks - 1, 1, 0), 4)
    prev_node = lax.rem(node + jnp.where(zh == 0, 3, 0), 4)
    ring = [(next_harm, next_node), (prev_harm, prev_node)]

    barrier = pltpu.get_barrier_semaphore()

    def greet(other, _):
        pl.semaphore_signal(barrier, inc=1, device_id=(other, node), device_id_type=MESH)

    each_peer(greet)
    for d in (1, 2, 3):
        pl.semaphore_signal(
            barrier, inc=1, device_id=(harm, lax.rem(node + d, 4)), device_id_type=MESH
        )
    for place in ring:
        pl.semaphore_signal(barrier, inc=1, device_id=place, device_id_type=MESH)
    is_last, is_first = mine == group - 1, mine == 0

    @pl.when(zh == 0)
    def _():
        place = (48 + (chunks - 1) * 2 + 1, prev_node)
        pl.semaphore_signal(barrier, inc=1, device_id=place, device_id_type=MESH)

    @pl.when(zh == chunks - 1)
    def _():
        pl.semaphore_signal(barrier, inc=1, device_id=(0, next_node), device_id_type=MESH)

    greeters = 68 + jnp.where(is_last & (zh == chunks - 1) | is_first & (zh == 0), group, 0)

    def copy(src, dst, ssem, rsem, place):
        return pltpu.make_async_remote_copy(
            src_ref=src, dst_ref=dst, send_sem=ssem, recv_sem=rsem,
            device_id=place, device_id_type=MESH,
        )

    def unit(index):
        return pl.ds(pl.multiple_of(index * 4, 4), 4)

    def exchange(bufs, at):
        send, recv, ssem, rsem = bufs

        def push(other, other_slot):
            copy(
                send.at[*at, unit(other_slot)], recv.at[*at, unit(slot)],
                ssem.at[0], rsem.at[*at], (other, node),
            ).start()

        each_peer(push)
        recv[*at, unit(slot), :] = send[*at, unit(slot), :]

    def exchanged(bufs, at):
        send, recv, ssem, rsem = bufs
        rows = pl.ds(0, 252)
        return copy(
            send.at[*at, rows], recv.at[*at, rows], ssem.at[0], rsem.at[*at], (prev_harm, node)
        )

    wide = 4 * chunks

    def share(bufs, at):
        send, recv, ssem, rsem = bufs
        own = pl.ds(pl.multiple_of(mine * wide, wide), wide)

        def push(other, place):
            copy(
                send.at[*at, pl.ds(pl.multiple_of(place * wide, wide), wide)], recv.at[*at, own],
                ssem.at[0], rsem.at[*at], (other, node),
            ).start()

        each_mate(push)
        recv[*at, own, :] = send[*at, own, :]

    def shared(bufs, at):
        send, recv, ssem, rsem = bufs
        rows = pl.ds(0, 256 - wide)
        return copy(
            send.at[*at, rows], recv.at[*at, rows],
            ssem.at[0], rsem.at[*at], (prev_harm, node),
        )

    def spread(c, q):
        return pl.ds(c * 4 + q, group, stride=wide)

    ta = (ta_send, ta_recv, ta_ssem, ta_rsem)
    la = (la_send, la_recv, la_ssem, la_rsem)
    zf = (ta_recv.at[1], zf_recv, zf_ssem, zf_rsem)
    lg = (lg_send, lg_recv, lg_ssem, lg_rsem)
    tg = (tg_send, tg_recv, tg_ssem, tg_rsem)

    def halo_copy(side):
        step = 1 if side == 0 else 3
        return copy(
            halo_send.at[side], halo_recv.at[side], h_ssem.at[0], h_rsem.at[0],
            (harm, lax.rem(node + step, 4)),
        )

    halo_both = copy(halo_send, halo_recv, h_ssem.at[0], h_rsem.at[0], ring[0])

    def ring_copy(stage, side):
        return copy(
            ring_send.at[stage, side], ring_recv.at[stage, side],
            r_ssem.at[0], r_rsem.at[stage], ring[side],
        )

    def edge_rows(side):
        high = lax.rem(zh + (1 if side == 0 else chunks - 1), chunks)
        beside = next_node if side == 0 else prev_node
        for place in range(group):
            copy(
                ta_recv.at[1, 1 - side, pl.ds(place * wide, wide)], ring_recv.at[0, side],
                r_ssem.at[1], r_rsem.at[0], (place // 2 * 16 + high * 2 + place % 2, beside),
            ).start()

    def ring_both(stage):
        return copy(
            ring_send.at[stage], ring_recv.at[stage], r_ssem.at[0], r_rsem.at[stage], ring[0]
        )

    pairs = [(p, kk) for p in range(2) for kk in range(2)]
    deep = 2 * group

    def strip(chunk, half):
        return slice(chunk * deep + half * group, chunk * deep + (half + 1) * group)

    def to_time(field, stage, half):
        for p, kk in pairs:
            for c in range(chunks):
                ta_send[stage, half, spread(c, p * 2 + kk), :] = field[p, kk, strip(c, half), :]

    def product(matrix, x):
        high, low = split(x)
        all_parts = jnp.dot(
            matrix[...], jnp.concatenate([high, low], axis=1), preferred_element_type=F32
        )
        return (all_parts[0:256, 0:128] + all_parts[0:256, 128:256]) + all_parts[256:512, 0:128]

    loads[0].wait()
    to_time(state, 0, 0)
    loads[1].wait()
    for kk in range(2):
        gathered[zh, kk, :, 0:128] = precond[0, kk].T
        gathered[zh, kk, :, 128:256] = precond[1, kk].T

    def build(high_place):
        for kk in range(2):
            high, low = split(gathered[high_place, kk])
            weights[high_place, kk, 0:128, :] = high
            weights[high_place, kk, 128:256, :] = low

    build(zh)
    for load in loads[2:]:
        load.wait()
    params = []
    for half in range(2):
        kind = kinds[pl.ds(zh * deep + half * group + mine, 1), :]
        params.append(
            [
                sum(jnp.where(kind == member, table[what, member], 0.0) for member in range(TYPES))
                for what in range(3)
            ]
        )
    shifts[...] = jnp.broadcast_to(shift[...].astype(F32), (128, 128)).T

    pl.semaphore_wait(barrier, greeters)
    exchange(ta, (0, 0))
    to_time(state, 0, 1)
    exchange(ta, (0, 1))
    last = [state[p, kk, 127:128, :] for p, kk in pairs]
    first = [state[p, kk, 0:1, :] for p, kk in pairs]
    halo_send[0] = jnp.concatenate(last + last, axis=0)
    halo_send[1] = jnp.concatenate(first + first, axis=0)
    for side in range(2):
        halo_copy(side).start()

    quarter = pl.ds(pl.multiple_of(node * 32, 32), 32)

    def along_z(way, step):
        high = along(step - 1 if way else chunks - (step - 1) if step > 1 else 0)[1]
        place = gathered.at[high, :, quarter]
        target = along(chunks - 1 if way else 1)[0]
        return copy(place, place, gz_ssem.at[0], gz_rsem.at[step - 1], (target, node))

    def along_x(way, step, dx):
        high = along(step if way else chunks - step)[1]
        place = gathered.at[high, :, quarter]
        return copy(
            place, place, gx_ssem.at[0], gx_rsem.at[step - 1], (harm, lax.rem(node + dx, 4))
        )

    def bulk(count, rows, ssem, rsem):
        place = gathered.at[pl.ds(0, count), :, pl.ds(0, rows)]
        return copy(place, place, ssem, rsem, (prev_harm, node))

    moves = [(way, step) for step in (1, 2, 3, 4) for way in (0, 1) if way == 0 or step < 4]

    def pass_on(step):
        ways = 2 if step < 4 else 1
        bulk(ways, 32, gz_ssem.at[0], gz_rsem.at[step - 1]).wait_recv()
        for way, at in moves:
            if at == step + 1:
                along_z(way, at).start()
        for dx in (2, 1, 3) if step != 3 else (1, 3):
            for way, at in moves:
                if at == step:
                    along_x(way, at, dx).start()

    def pass_rest():
        rows = pl.ds(pl.multiple_of(lax.rem(node + 2, 4) * 32, 32), 32)
        for way in (0, 1):
            place = gathered.at[along(2 if way else chunks - 2)[1], :, rows]
            target = along(chunks - 1 if way else 1)[0]
            copy(place, place, gx_ssem.at[0], gx_rsem.at[2], (target, node)).start()

    def receive(step):
        ways = 2 if step < 4 else 1
        bulk(ways, 96, gx_ssem.at[0], gx_rsem.at[step - 1]).wait_recv()
        for way, at in moves:
            if at == step:
                build(along(at if way else chunks - at)[1])

    for way, at in moves:
        if at == 1:
            along_z(way, at).start()

    def stencil(f, turned, halo_a, halo_b, shift_rows):
        rows = f.shape[0]
        row = lax.broadcasted_iota(jnp.int32, (rows, 128), 0)
        above = jnp.where(row == 0, halo_a, pltpu.roll(f, 1, axis=0))
        below = jnp.where(row == rows - 1, halo_b, pltpu.roll(f, rows - 1, axis=0))
        skewed = above
        for amount in range(1, SHIFTS):
            skewed = jnp.where(
                shift_rows == float(amount), pltpu.roll(above, 128 - amount, axis=1), skewed
            )
        sides = pltpu.roll(f, 1, axis=1) + pltpu.roll(f, 127, axis=1)
        return 4.0 * f - sides - skewed - below + turned

    zero = jnp.zeros((128, 128), BF16)

    def complex_product(u0, u1, weight):
        rows = u0.shape[0]
        high, low = split(jnp.concatenate([u0, u1], axis=0))
        left = jnp.concatenate(
            [
                jnp.concatenate([high, high], axis=1),
                jnp.concatenate([low, zero[0 : 2 * rows]], axis=1),
            ],
            axis=0,
        )
        out = jnp.dot(left, weight, preferred_element_type=F32)
        out = out[0 : 2 * rows] + out[2 * rows : 4 * rows]
        real = out[0:rows, 0:128] - out[rows : 2 * rows, 128:256]
        imag = out[0:rows, 128:256] + out[rows : 2 * rows, 0:128]
        return real, imag

    def evaluate(half):
        linear, amplitude, slope = params[half]
        exchanged(ta, (0, half)).wait_recv()
        voltage = product(inv, ta_recv[0, half])
        bent = jnp.tanh(slope * voltage)
        slopes[half] = linear + amplitude * slope * (1.0 - bent * bent)
        la_send[half] = product(fwd, linear * voltage + amplitude * bent)
        exchange(la, (half,))

    evaluate(0)
    halo_both.wait_recv()
    not_first = jnp.where(node == 0, 0.0, 1.0)
    not_last = jnp.where(node == 3, 0.0, 1.0)
    for p, kk in pairs:
        index = p * 2 + kk
        wave = (2 * harm + kk).astype(F32) * (-OMEGA if p == 0 else OMEGA)
        start[index] = source[p, kk] - stencil(
            state[p, kk],
            wave * cap[...] * state[1 - p, kk],
            halo_recv[0, index : index + 1, :] * not_first,
            halo_recv[1, index : index + 1, :] * not_last,
            shifts[...],
        )
    evaluate(1)
    pass_on(1)
    for half in range(2):
        exchanged(la, (half,)).wait_recv()
        for q in range(4):
            for c in range(chunks):
                part = strip(c, half)
                start[q, part, :] = start[q, part, :] - la_recv[half, spread(c, q), :]
        for kk in range(2):
            u0, u1 = [
                jnp.concatenate([start[q, strip(c, half), :] for c in range(chunks)], axis=0)
                for q in (kk, 2 + kk)
            ]
            real, imag = complex_product(u0, u1, weights[zh, kk])
            for q, value in ((kk, real), (2 + kk, imag)):
                for c in range(chunks):
                    piece = value[c * group : (c + 1) * group]
                    ta_send[1, half, spread(c, q), :] = piece
                    first_z[q, strip(c, half), :] = piece
        exchange(ta, (1, half))
        if half == 0:
            pass_on(2)
    receive(1)
    for p, kk in pairs:
        out_resid[p, kk] = -start[p * 2 + kk]
    resid_out = pltpu.make_async_copy(out_resid, resid_hbm, out_sem.at[1])
    resid_out.start()
    def to_spec(signal, stage, half):
        lg_send[stage, half] = product(fwd, signal)
        share(lg, (stage, half))

    for half in range(2):
        exchanged(ta, (1, half)).wait_recv()
        share(zf, (half,))
        pl.when(is_last if half else is_first)(functools.partial(edge_rows, 1 - half))
        to_spec(slopes[half] * product(inv, ta_recv[1, half]), 0, half)
        pass_on(3 + half)
    receive(2)
    pass_rest()

    def start_copy(d):
        other, high = along(d)
        return copy(
            start.at[:, pl.ds(pl.multiple_of(high * deep, deep), deep)], start_rows.at[zh],
            b_ssem.at[0], b_rsem.at[0], (other, node),
        )

    def back_copy(which, d):
        other, high = along(d)
        size = 4 * deep
        return copy(
            direct.at[which, pl.ds(pl.multiple_of(high * size, size), size)],
            direct_back.at[which - 1, pl.ds(pl.multiple_of(zh * size, size), size)],
            b_ssem.at[1], b_rsem.at[1], (other, node),
        )

    start_rows[zh] = start[:, pl.ds(pl.multiple_of(zh * deep, deep), deep), :]

    rows_of_others = start_rows.at[pl.ds(0, chunks - 1)]
    start_all = copy(
        rows_of_others, rows_of_others, b_ssem.at[0], b_rsem.at[0], (prev_harm, node)
    )
    back_of_others = direct_back.at[:, pl.ds(0, 512 - 4 * deep)]
    back_all = copy(
        back_of_others, back_of_others, b_ssem.at[1], b_rsem.at[1], (prev_harm, node)
    )

    fields = [(c, q) for c in range(chunks) for q in range(4)]

    def at_rows(c, q, half=None):
        first_row = (c * 4 + q) * deep
        if half is None:
            return pl.ds(first_row, deep)
        return pl.ds(first_row + half * group, group)

    def send_ring(which):
        ring_send[which, 0] = direct[which, pl.ds(deep - 1, 4 * chunks, stride=deep), :]
        ring_send[which, 1] = direct[which, pl.ds(0, 4 * chunks, stride=deep), :]
        for side in range(2):
            ring_copy(which, side).start()

    chunk = pl.ds(pl.multiple_of(zh * deep, deep), deep)
    has_above = jnp.where((node == 0) & (zh == 0), 0.0, 1.0)
    has_below = jnp.where((node == 3) & (zh == chunks - 1), 0.0, 1.0)

    def local_image(which):
        ring_both(which).wait_recv()
        cap_rows, shift_rows = cap[chunk, :], shifts[chunk, :]
        for c, q in fields:
            p, kk = q // 2, q % 2
            place = y * 16 + (c * FOLD + zl) * 2 + core
            wave = (2 * place + kk).astype(F32) * (-OMEGA if p == 0 else OMEGA)
            index = c * 4 + q
            images[which, at_rows(c, q), :] = stencil(
                direct[which, at_rows(c, q), :],
                wave * cap_rows * direct[which, at_rows(c, (q + 2) % 4), :],
                ring_recv[which, 0, index : index + 1, :] * has_above,
                ring_recv[which, 1, index : index + 1, :] * has_below,
                shift_rows,
            )

    def finish_image(which, half):
        shared(lg, (which, half)).wait_recv()
        for c, q in fields:
            rows = at_rows(c, q, half)
            value = images[which, rows, :] + lg_recv[which, half, spread(c, q), :]
            if which > 0:
                value = value - images[which - 1, rows, :]
            images[which, rows, :] = value

    def send_direction(which, half):
        for c in range(chunks):
            for kk in range(2):
                real, imag = complex_product(
                    images[which - 1, at_rows(c, kk, half), :],
                    images[which - 1, at_rows(c, 2 + kk, half), :],
                    weights[c, kk],
                )
                for q, value in ((kk, real), (2 + kk, imag)):
                    direct[which, at_rows(c, q, half), :] = value
                    tg_send[which - 1, half, spread(c, q), :] = value
        share(tg, (which - 1, half))

    def inner(a, b, half):
        total = jnp.zeros((8, 128), F32)
        for c, q in fields:
            term = a(c, q, half) * b(c, q, half)
            for i in range(group // 8):
                total = total + term[i * 8 : (i + 1) * 8]
        return total

    def image_rows(which):
        return lambda c, q, half: images[which, at_rows(c, q, half), :]

    def start_part(c, q, half):
        return start_rows[c, q, half * group : (half + 1) * group, :]

    def closed(total):
        return jnp.sum(jnp.sum(total, axis=0, keepdims=True), axis=1, keepdims=True)

    for half in range(2):
        shared(zf, (half,)).wait_recv()
        for c, q in fields:
            direct[0, at_rows(c, q, half), :] = zf_recv[half, spread(c, q), :]
    for d in range(1, chunks):
        start_copy(d).start()
    receive(3)
    receive(4)
    local_image(0)

    dots = {}
    for which in (1, 2):
        for half in range(2):
            finish_image(which - 1, half)
            send_direction(which, half)
        send_ring(which)
        for d in range(1, chunks):
            back_copy(which, d).start()
        size = 4 * deep
        own = pl.ds(pl.multiple_of(zh * size, size), size)
        direct_back[which - 1, own, :] = direct[which, own, :]
        for half in range(2):
            shared(tg, (which - 1, half)).wait_recv()
            to_spec(slopes[half] * product(inv, tg_recv[which - 1, half]), which, half)
        local_image(which)
        if which == 1:
            start_all.wait_recv()
        now = image_rows(which - 1)
        for name, other in [("start", start_part)] + [(j, image_rows(j)) for j in range(which)]:
            dots[name, which - 1] = closed(inner(other, now, 0) + inner(other, now, 1))
    others = [("start", start_part)] + [(j, image_rows(j)) for j in range(3)]
    sums = []
    for half in range(2):
        finish_image(2, half)
        sums.append([inner(other, image_rows(2), half) for _, other in others])
    for (name, _), one, two in zip(others, *sums):
        dots[name, 2] = closed(one + two)

    names = list(dots)
    lane = lax.broadcasted_iota(jnp.int32, (1, 128), 1)
    packed = sum(jnp.where(lane == i, dots[name], 0.0) for i, name in enumerate(names))
    ar_send[...] = packed

    def push(other, _):
        copy(ar_send, ar_recv.at[harm], a_ssem.at[0], a_rsem.at[0], (other, node)).start()

    each_peer(push)
    ar_recv[harm] = packed
    all_sums = copy(
        ar_recv.at[pl.ds(0, 63)], ar_recv.at[pl.ds(0, 63)], a_ssem.at[0], a_rsem.at[0],
        (prev_harm, node),
    )
    def left(part, ssem):
        copy(part, part, ssem, a_rsem.at[0], (prev_harm, node)).wait_send()

    left(ta_send.at[:, :, pl.ds(0, 252)], ta_ssem.at[0])
    left(la_send.at[:, pl.ds(0, 252)], la_ssem.at[0])
    left(zf_recv.at[:, pl.ds(0, 256 - wide)], zf_ssem.at[0])
    left(lg_send.at[:, :, pl.ds(0, 256 - wide)], lg_ssem.at[0])
    left(tg_send.at[:, :, pl.ds(0, 256 - wide)], tg_ssem.at[0])
    left(ring_send.at[pl.ds(1, 2)], r_ssem.at[0])

    @pl.when(is_last | is_first)
    def _():
        left(ta_recv.at[1, 0], r_ssem.at[1])

    halo_both.wait_send()
    bulk(7, 32, gz_ssem.at[0], gz_rsem.at[0]).wait_send()
    bulk(7, 96, gx_ssem.at[0], gx_rsem.at[0]).wait_send()
    start_all.wait_send()
    back_all.wait_send()
    all_sums.wait_recv()
    total = jnp.sum(ar_recv[...], axis=0)
    ax_send[...] = total

    def ax_copy(dx):
        return copy(
            ax_send, ax_recv.at[node], x_ssem.at[0], x_rsem.at[0],
            (harm, lax.rem(node + dx, 4)),
        )

    for dx in (1, 2, 3):
        ax_copy(dx).start()
    ax_recv[node] = total
    back_all.wait_recv()
    ax_all = copy(
        ax_recv.at[pl.ds(0, 3)], ax_recv.at[pl.ds(0, 3)], x_ssem.at[0], x_rsem.at[0], ring[0]
    )
    ax_all.wait_recv()
    total = jnp.sum(ax_recv[...], axis=0)
    value = {name: total[:, i : i + 1] for i, name in enumerate(names)}

    g00, g01, g02 = value[0, 0], value[0, 1], value[0, 2]
    g11, g12, g22 = value[1, 1], value[1, 2], value[2, 2]
    b0, b1, b2 = value["start", 0], value["start", 1], value["start", 2]
    l10, l20 = g01 / g00, g02 / g00
    d1 = g11 - l10 * g01
    e12 = g12 - l10 * g02
    c1 = b1 - l10 * b0
    l21 = e12 / d1
    d2 = g22 - l20 * g02 - l21 * e12
    c2 = b2 - l20 * b0 - l21 * c1
    y2 = c2 / d2
    y1 = (c1 - e12 * y2) / d1
    y0 = (b0 - g01 * y1 - g02 * y2) / g00
    w0, w1, w2 = y0 - y1 + y2, y1 - y2, y2
    for p, kk in pairs:
        q = p * 2 + kk
        for c in range(chunks):
            rows = slice(c * deep, (c + 1) * deep)
            out_update[p, kk, rows, :] = (
                w0 * first_z[q, rows, :]
                + w1 * direct_back[0, at_rows(c, q), :]
                + w2 * direct_back[1, at_rows(c, q), :]
            )
        pltpu.make_async_copy(out_update.at[p, kk], update_hbm.at[p, kk], out_sem.at[0]).start()

    all_sums.wait_send()
    ax_all.wait_send()
    pltpu.make_async_copy(out_update, update_hbm, out_sem.at[0]).wait()
    resid_out.wait()


def hand_over(update, resid, update_out, resid_out, held, in_sem, out_sem):
    ways = [(update, update_out), (resid, resid_out)]
    loads = [pltpu.make_async_copy(a, held.at[i], in_sem.at[i]) for i, (a, _) in enumerate(ways)]
    stores = [pltpu.make_async_copy(held.at[i], b, out_sem.at[i]) for i, (_, b) in enumerate(ways)]
    for load in loads:
        load.start()
    for load, store in zip(loads, stores):
        load.wait()
        store.start()
    for store in stores:
        store.wait()


def body(state, source, capacity, row_shift, device_type, device_table, precond):
    inverse, forward = tables(state.shape[1] * lax.axis_size("harm"))
    block = (2, 2, 128, 128)
    chunks, group = 8 // FOLD, 8 * FOLD
    vmem = pltpu.VMEM
    dma = pltpu.SemaphoreType.DMA
    hbm = pl.BlockSpec(memory_space=pltpu.HBM)

    def four(*lead):
        return [vmem(lead + (256, 128), F32)] * 2

    update, resid = pl.pallas_call(
        kernel,
        out_shape=[jax.ShapeDtypeStruct(block, F32)] * 2,
        in_specs=[hbm] * 5 + [pl.BlockSpec(memory_space=pltpu.SMEM)] + [hbm] * 3,
        out_specs=[hbm] * 2,
        scratch_shapes=[
            vmem(block, F32), vmem(block, F32), vmem((128, 128), F32), vmem((1, 128), jnp.int32),
            vmem((128, 128), jnp.int32), vmem(block, F32), vmem((512, 256), BF16),
            vmem((512, 256), BF16),
            vmem((chunks, 2, 128, 256), F32), vmem((chunks, 2, 256, 256), BF16),
            vmem((2, 256, 128), F32), vmem((128, 128), F32), vmem((4, 128, 128), F32),
            vmem((chunks, 4, 2 * group, 128), F32), vmem((4, 128, 128), F32),
            vmem((3, 512, 128), F32), vmem((3, 512, 128), F32), vmem((2, 512, 128), F32),
            vmem(block, F32), vmem(block, F32),
            *four(2, 2), *four(2), vmem((2, 256, 128), F32), *four(3, 2), *four(2, 2),
            vmem((2, 8, 128), F32), vmem((2, 8, 128), F32),
            vmem((3, 2, 4 * chunks, 128), F32), vmem((3, 2, 4 * chunks, 128), F32),
            vmem((1, 128), F32), vmem((64, 1, 128), F32),
            vmem((1, 128), F32), vmem((4, 1, 128), F32),
            dma((8,)), dma((2,)), dma((1,)), dma((2, 2)), dma((1,)), dma((2,)), dma((1,)),
            dma((2,)), dma((1,)), dma((3, 2)), dma((1,)), dma((2, 2)), dma((1,)), dma((1,)),
            dma((2,)), dma((3,)), dma((1,)), dma((4,)), dma((1,)), dma((4,)), dma((2,)),
            dma((2,)), dma((1,)), dma((1,)), dma((1,)), dma((1,)),
        ],
        compiler_params=pltpu.CompilerParams(
            collective_id=0, has_side_effects=True, vmem_limit_bytes=67_000_000
        ),
    )(
        state, source, capacity, row_shift.reshape(1, -1), device_type, device_table, precond,
        jnp.asarray(inverse), jnp.asarray(forward),
    )
    return pl.pallas_call(
        hand_over,
        out_shape=[jax.ShapeDtypeStruct(block, F32)] * 2,
        in_specs=[hbm] * 2,
        out_specs=[hbm] * 2,
        scratch_shapes=[vmem((2,) + block, F32), dma((2,)), dma((2,))],
        compiler_params=pltpu.CompilerParams(vmem_limit_bytes=67_000_000),
    )(update, resid)


def solution(mesh):
    harm, node = mesh.axis_names
    return jax.shard_map(
        body,
        mesh=mesh,
        in_specs=(
            P(None, harm, node, None),
            P(None, harm, node, None),
            P(node, None),
            P(node),
            P(node, None),
            P(),
            P(None, harm, None, None),
        ),
        out_specs=(P(None, harm, node, None), P(None, harm, node, None)),
        check_vma=False,
    )
```
